256 devices in a mesh: section: 16 (over z_lo, x), tensor: 16 (over z_hi, y, core).
Axes of the slice: x: 4, y: 4, z: 8 (z_hi: 2, z_lo: 4; z = z_hi * 4 + z_lo), core: 2. Of those that a mesh axis runs over, the one named last changes fastest.
Arguments:
- layer_input: bfloat16 [6144, 5120], P('section', 'tensor'), may hold values from -6 to 6
- query_rows: bfloat16 [6144, 4096], P('section', 'tensor'), may hold values from -4.6 to 4.6
- key_rows: bfloat16 [6144, 4096], P('section', 'tensor'), may hold values from -4.6 to 4.6
- value_rows: bfloat16 [6144, 4096], P('section', 'tensor'), may hold values from -6 to 6
- out_grad: bfloat16 [6144, 5120], P('section', 'tensor'), may hold values from -6 to 6
- window: int32 [32], P('tensor'), may hold values from 96 to 192, as said below
- w_query: bfloat16 [5120, 4096], P(None, 'tensor'), may hold values from -0.078125 to 0.078125
- w_key: bfloat16 [5120, 4096], P(None, 'tensor'), may hold values from -0.078125 to 0.078125
- w_value: bfloat16 [5120, 4096], P(None, 'tensor'), may hold values from -0.078125 to 0.078125
- w_out: bfloat16 [4096, 5120], P('tensor'), may hold values from -0.09375 to 0.09375
Outputs:
- input_grad: bfloat16 [6144, 5120], P('section', 'tensor')
- query_weight_grad: float32 [5120, 4096], P('section', 'tensor')
- key_weight_grad: float32 [5120, 4096], P('section', 'tensor')
- value_weight_grad: float32 [5120, 4096], P('section', 'tensor')
- out_weight_grad: float32 [4096, 5120], P('tensor', 'section')
The draws below stay inside these ranges and needn't reach their ends.
Inputs may be any that keep to these rules, and one draw needn't show every extreme that they name: `window`: the number of most recent positions, the query's own included, that a head sees; some head has exactly 192.
All inputs are finite; a program needn't handle non-finite values.
Results may differ from the reference program's by a relative error of at most 0.025.
Values may be sent and summed in bfloat16 or wider, within the bound.
A program may use at most 128 MiB of HBM per device.

```python
import math
import jax
import jax.numpy as jnp
from jax import lax

D = 5120
HEADS = 32
HD = 128
WMAX = 192
TOK_DEV = 384
TOKENS = 6144
N_SECTION = 16


def paired_rows(key):
    shape = (TOKENS, HEADS * HD)
    base_query = jnp.clip(jax.random.normal(jax.random.fold_in(key, 11), shape, jnp.float32), -4.6, 4.6)
    base_key = jnp.clip(jax.random.normal(jax.random.fold_in(key, 12), shape, jnp.float32), -4.6, 4.6)
    return (base_query, base_key)


def draw_query_rows(key, part):
    return paired_rows(key)[0].astype(jnp.bfloat16)


def draw_key_rows(key, part):
    return paired_rows(key)[1].astype(jnp.bfloat16)


def draw_window(key, part):
    lengths = jax.random.randint(jax.random.fold_in(key, 21), (HEADS,), WMAX // 2, WMAX + 1)
    chosen = jax.random.randint(jax.random.fold_in(key, 22), (), 0, HEADS)
    return jnp.where(jnp.arange(HEADS) == chosen, WMAX, lengths).astype(jnp.int32)


def steps_of(own_key, extent, shards, smallest, high):
    def one(position, shards_of):
        draws = jax.random.uniform(jax.random.fold_in(jax.random.fold_in(own_key, 6), position), (shards_of,), jnp.float32, smallest / len(shards), high / len(shards))
        return jnp.repeat(jnp.exp(draws), extent[position] // shards_of).reshape((-1,) + (1,) * (len(extent) - position - 1))

    loudness = one(*shards[0])
    for cut in shards[1:]:
        loudness = loudness * one(*cut)
    return loudness


def bell_draw(key, dims, width, reach, pieces=(), kind=jnp.bfloat16):
    values = width * jax.random.normal(key, dims, jnp.float32)
    if pieces:
        values = values * steps_of(key, dims, pieces, -0.22, 0.18)
    return jnp.clip(values, -reach, reach).astype(kind)


def setup_inputs(seed: int = 0) -> dict:
    splits = jax.random.split(jax.random.key(seed), 11)
    return {
        "layer_input": bell_draw(splits[0], (TOKENS, D), 1.0, 6.0, ((0, 16), (1, 16))),
        "query_rows": draw_query_rows(jax.random.fold_in(splits[10], 71), 0),
        "key_rows": draw_key_rows(jax.random.fold_in(splits[10], 71), 0),
        "value_rows": bell_draw(splits[3], (TOKENS, HEADS * HD), 1.0, 6.0, ((0, 16), (1, 16))),
        "out_grad": bell_draw(splits[4], (TOKENS, D), 1.0, 6.0, ((0, 16), (1, 16))),
        "window": draw_window(jax.random.fold_in(splits[10], 71), 0),
        "w_query": bell_draw(splits[6], (D, HEADS * HD), D ** -0.5, 0.078125, ((1, 16),)),
        "w_key": bell_draw(splits[7], (D, HEADS * HD), D ** -0.5, 0.078125, ((1, 16),)),
        "w_value": bell_draw(splits[8], (D, HEADS * HD), D ** -0.5, 0.078125, ((1, 16),)),
        "w_out": bell_draw(splits[9], (HEADS * HD, D), (HEADS * HD) ** -0.5, 0.09375, ((0, 16),)),
    }


def window_backward(query_rows, key_rows, value_rows, grad_rows, window, first_row):
    row_count = query_rows.shape[0]
    key_count = key_rows.shape[0]
    span = key_count - row_count
    head_count = query_rows.shape[1] // HD
    scaling = 1.0 / math.sqrt(HD)
    query_heads = query_rows.reshape(row_count, head_count, HD).astype(jnp.float32)
    key_heads = key_rows.reshape(key_count, head_count, HD).astype(jnp.float32)
    value_heads = value_rows.reshape(key_count, head_count, HD).astype(jnp.float32)
    grad_heads = grad_rows.reshape(row_count, head_count, HD).astype(jnp.float32)
    query_pos = first_row + jnp.arange(row_count, dtype=jnp.int32)
    key_pos = first_row - span + jnp.arange(key_count, dtype=jnp.int32)
    distance = query_pos[:, None] - key_pos[None, :]
    visible = (distance[None] >= 0) & (distance[None] < window[:, None, None]) & (key_pos[None, None, :] >= 0)
    scores = jnp.einsum('thd,khd->htk', query_heads, key_heads) * scaling
    scores = jnp.where(visible, scores, -jnp.inf)
    row_max = lax.optimization_barrier(jnp.max(scores, axis=2, keepdims=True))
    expon = jnp.exp(scores - row_max)
    probs = expon / lax.optimization_barrier(jnp.sum(expon, axis=2, keepdims=True))
    probs_low = probs.astype(jnp.bfloat16)
    attended = jnp.einsum('htk,khd->thd', probs_low.astype(jnp.float32), value_heads).astype(jnp.bfloat16)
    prob_grad = jnp.einsum('thd,khd->htk', grad_heads, value_heads)
    row_term = lax.optimization_barrier(jnp.sum(grad_heads * attended.astype(jnp.float32), axis=2))
    score_grad = (probs * (prob_grad - jnp.transpose(row_term)[:, :, None])).astype(jnp.bfloat16)
    score_wide = score_grad.astype(jnp.float32)
    grad_query = jnp.einsum('htk,khd->thd', score_wide, key_heads) * scaling
    grad_key = jnp.einsum('htk,thd->khd', score_wide, query_heads) * scaling
    grad_value = jnp.einsum('htk,thd->khd', probs_low.astype(jnp.float32), grad_heads)
    cols = head_count * HD
    return (attended.reshape(row_count, cols), grad_query.reshape(row_count, cols), grad_key.reshape(key_count, cols), grad_value.reshape(key_count, cols))

def reference(layer_input, query_rows, key_rows, value_rows, out_grad, window, w_query, w_key, w_value, w_out):
    cols = query_rows.shape[1]
    head_grad = jnp.dot(out_grad, w_out.T, preferred_element_type=jnp.float32).astype(jnp.bfloat16)
    padding = jnp.zeros((WMAX, cols), jnp.bfloat16)
    key_pad = jnp.concatenate([padding, key_rows], axis=0)
    value_pad = jnp.concatenate([padding, value_rows], axis=0)

    def one_block(block):
        start = (block * TOK_DEV).astype(jnp.int32)
        query_part = lax.dynamic_slice_in_dim(query_rows, start, TOK_DEV, 0)
        grad_part = lax.dynamic_slice_in_dim(head_grad, start, TOK_DEV, 0)
        key_part = lax.dynamic_slice_in_dim(key_pad, start, WMAX + TOK_DEV, 0)
        value_part = lax.dynamic_slice_in_dim(value_pad, start, WMAX + TOK_DEV, 0)
        return window_backward(query_part, key_part, value_part, grad_part, window, start)
    attended, grad_query, grad_key, grad_value = lax.map(one_block, jnp.arange(N_SECTION, dtype=jnp.int32))

    def carried(parts):
        later = jnp.concatenate([parts[1:, :WMAX], jnp.zeros((1, WMAX, cols), parts.dtype)], axis=0)
        own = parts[:, WMAX:]
        own = own.at[:, TOK_DEV - WMAX:].add(later)
        return own.reshape(TOKENS, cols).astype(jnp.bfloat16)
    attended = attended.reshape(TOKENS, cols)
    query_grad = grad_query.reshape(TOKENS, cols).astype(jnp.bfloat16)
    key_grad = carried(grad_key)
    value_grad = carried(grad_value)
    summed = jnp.dot(query_grad, w_query.T, preferred_element_type=jnp.float32)
    summed = summed + jnp.dot(key_grad, w_key.T, preferred_element_type=jnp.float32)
    summed = summed + jnp.dot(value_grad, w_value.T, preferred_element_type=jnp.float32)
    input_grad = summed.astype(jnp.bfloat16)
    query_weight_grad = jnp.dot(layer_input.T, query_grad, preferred_element_type=jnp.float32)
    key_weight_grad = jnp.dot(layer_input.T, key_grad, preferred_element_type=jnp.float32)
    value_weight_grad = jnp.dot(layer_input.T, value_grad, preferred_element_type=jnp.float32)
    out_weight_grad = jnp.dot(attended.T, out_grad, preferred_element_type=jnp.float32)
    return (input_grad, query_weight_grad, key_weight_grad, value_weight_grad, out_weight_grad)
```

```python
import math

import jax
import jax.numpy as jnp
from jax import lax
from jax.experimental import pallas as pl
from jax.experimental.pallas import tpu as pltpu
from jax.sharding import PartitionSpec as P

HD = 128
WMAX = 192
ROWS = 384
COLS = 256
SHARD = 320
PAD = 64
KEYS = PAD + WMAX + ROWS
BLOCK = 128
SPAN = 384
SEMS = 160
MESH = pl.DeviceIdType.MESH
BF = jnp.bfloat16
F32 = jnp.float32


def mm(a, b):
    return jnp.dot(a, b, preferred_element_type=F32)


def mm_nt(a, b):
    return lax.dot_general(a, b, (((1,), (1,)), ((), ())), preferred_element_type=F32)


def mm_tn(a, b):
    return lax.dot_general(a, b, (((0,), (0,)), ((), ())), preferred_element_type=F32)


class Wire:
    def __init__(self, send_sem, recv_sem, someone):
        self.send_sem, self.recv_sem, self.someone = send_sem, recv_sem, someone
        self.index = {}
        self.sent = []

    def copy(self, name, src, dst, device):
        i = self.index.setdefault(name, len(self.index))
        assert i < SEMS
        return pltpu.make_async_remote_copy(
            src_ref=src,
            dst_ref=dst,
            send_sem=self.send_sem.at[i],
            recv_sem=self.recv_sem.at[i],
            device_id=device,
            device_id_type=MESH,
        )

    def send(self, name, src, dst, device):
        c = self.copy(name, src, dst, device)
        c.start()
        self.sent.append(c)

    def recv(self, name, dst):
        self.copy(name, dst, dst, self.someone).wait_recv()

    def finish(self):
        for c in self.sent:
            c.wait_send()


def kernel(
    window,
    x_in,
    g_in,
    q_in,
    k_in,
    v_in,
    wq_in,
    wk_in,
    wv_in,
    wo_in,
    ig_out,
    dq_out,
    dk_out,
    dv_out,
    do_out,
    g_all,
    x_all,
    z_rel,
    w_all,
    wo,
    q,
    kcat,
    vcat,
    p_all,
    att,
    hg,
    dq,
    dk,
    dv,
    dk_acc,
    dv_acc,
    halo_out,
    halo_in,
    part,
    rel_l,
    rel_r,
    rec_l,
    rec_r,
    zs,
    zr,
    igp,
    d2r,
    yrel,
    yrec,
    zs_ig,
    zr_ig,
    send_sem,
    recv_sem,
    load_sem,
):
    section = lax.axis_index("section")
    tensor = lax.axis_index("tensor")
    zl, x = section // 4, lax.rem(section, 4)
    zh, y, c = tensor // 8, lax.rem(tensor // 2, 4), lax.rem(tensor, 2)
    zz = zh * 4 + zl
    way = 1 - 2 * c
    xr, xo, xl = lax.rem(x + 1, 4), lax.rem(x + 2, 4), lax.rem(x + 3, 4)
    yr, yo, yl = lax.rem(y + 1, 4), lax.rem(y + 2, 4), lax.rem(y + 3, 4)

    def at(x_=x, y_=y, zz_=zz, c_=c):
        return (lax.rem(zz_, 4) * 4 + x_, (zz_ // 4) * 8 + y_ * 2 + c_)

    def slot(zh_=zh, y_=y, c_=c):
        return zh_ * 8 + y_ * 2 + c_

    def zat(step):
        return at(zz_=lax.rem(zz + step + 8, 8))

    partner = at(c_=1 - c)
    y_right, y_left = at(y_=yr), at(y_=yl)
    x_right, x_left = at(x_=xr), at(x_=xl)
    z_far, z_next = zat(3 * way), zat(way)
    z_low = [(lax.rem(zl + d, 4) * 4 + x, tensor) for d in (1, 2, 3)]
    s_next = (lax.rem(section + 1, 16), tensor)
    s_prev = (lax.rem(section + 15, 16), tensor)

    loads = {}

    def load(name, src, dst):
        cp = pltpu.make_async_copy(src, dst, load_sem.at[len(loads)])
        loads[name] = cp
        cp.start()

    load("q", q_in, q)
    load("k", k_in, kcat.at[pl.ds(PAD + WMAX, ROWS)])
    load("v", v_in, vcat.at[pl.ds(PAD + WMAX, ROWS)])
    load("g", g_in, g_all.at[tensor])
    load("x", x_in, x_all.at[tensor])
    load("wo", wo_in, wo)
    load("wq", wq_in, w_all.at[0])
    load("wk", wk_in, w_all.at[1])
    load("wv", wv_in, w_all.at[2])

    barrier = pltpu.get_barrier_semaphore()
    peers = [partner, y_right, y_left, x_right, x_left, s_next, s_prev]
    peers += z_low + [zat(3), zat(-3), zat(1), zat(-1)]
    for peer in peers:
        pl.semaphore_signal(barrier, inc=1, device_id=peer, device_id_type=MESH)
    pl.semaphore_wait(barrier, len(peers))

    wire = Wire(send_sem, recv_sem, partner)
    send, recv = wire.send, wire.recv

    class Gather:
        def __init__(self, tag, own, buf, rel):
            self.tag, self.own, self.buf, self.rel = tag, own, buf, rel

        def start(self):
            mine = self.buf.at[tensor]
            send(self.tag + "L", self.own, mine, y_right)
            send(self.tag + "R", self.own, mine, y_left)
            send(self.tag + "Q", self.own, self.rel, z_far)
            send(self.tag + "P0", self.own, mine, partner)

        def half(self, s, i):
            return self.buf.at[s, pl.ds(160 * i, 160)]

        def sides(self, z, far, names):
            here = slot(far, yl)
            recv(self.tag + z + "L", self.buf.at[here])
            send(self.tag + z + "OA", self.half(here, 0), self.half(here, 0), y_right)
            send(self.tag + names[0], self.buf.at[here], self.buf.at[here], partner)
            here = slot(far, yr)
            recv(self.tag + z + "R", self.buf.at[here])
            send(self.tag + z + "OB", self.half(here, 1), self.half(here, 1), y_left)
            send(self.tag + names[1], self.buf.at[here], self.buf.at[here], partner)

        def opposite(self, z, far, name):
            here = slot(far, yo)
            recv(self.tag + z + "OA", self.half(here, 0))
            recv(self.tag + z + "OB", self.half(here, 1))
            send(self.tag + name, self.buf.at[here], self.buf.at[here], partner)

        def near_sides(self):
            self.sides("", zh, ("P1", "P2"))

        def near_opposite(self):
            self.opposite("", zh, "P3")

        def relay(self):
            recv(self.tag + "Q", self.rel)
            source = lax.rem(zz - 3 * way + 8, 8)
            here = self.buf.at[slot(source // 4)]
            send(self.tag + "Z", self.rel, here, z_next)

        def across(self):
            here = self.buf.at[slot(1 - zh)]
            recv(self.tag + "Z", here)
            send(self.tag + "ZL", here, here, y_right)
            send(self.tag + "ZR", here, here, y_left)
            send(self.tag + "P4", here, here, partner)

        def far_sides(self):
            self.sides("Z", 1 - zh, ("P5", "P6"))

        def far_opposite(self):
            self.opposite("Z", 1 - zh, "P7")

        def finish(self):
            for i in range(8):
                far = zh if i < 4 else 1 - zh
                where = (y, yl, yr, yo)[i % 4]
                recv(self.tag + "P" + str(i), self.buf.at[slot(far, where, 1 - c)])

    grad = Gather("g", g_in, g_all, z_rel.at[0])
    inp = Gather("x", x_in, x_all, z_rel.at[1])
    halo_rows = pl.ds(ROWS - WMAX, WMAX)
    send("hk", k_in.at[halo_rows], kcat.at[pl.ds(PAD, WMAX)], s_next)
    send("hv", v_in.at[halo_rows], vcat.at[pl.ds(PAD, WMAX)], s_next)
    grad.start()
    inp.start()

    scaling = 1.0 / math.sqrt(HD)
    zero_rows = jnp.zeros((PAD, COLS), BF)
    kcat[pl.ds(0, PAD)] = zero_rows
    vcat[pl.ds(0, PAD)] = zero_rows
    dk_acc[...] = jnp.zeros_like(dk_acc)
    dv_acc[...] = jnp.zeros_like(dv_acc)
    loads["q"].wait()
    loads["k"].wait()
    loads["v"].wait()
    recv("hk", kcat.at[pl.ds(PAD, WMAX)])
    recv("hv", vcat.at[pl.ds(PAD, WMAX)])
    first = section * ROWS

    def forward(b, carry):
        row = pl.multiple_of(b * BLOCK, BLOCK)
        i = lax.broadcasted_iota(jnp.int32, (BLOCK, SPAN), 0)
        j = lax.broadcasted_iota(jnp.int32, (BLOCK, SPAN), 1)
        distance = i + (PAD + WMAX) - j
        key_pos = first - (PAD + WMAX) + row + j
        for h in range(2):
            cols = pl.ds(h * HD, HD)
            keys = kcat[pl.ds(row, SPAN), cols]
            values = vcat[pl.ds(row, SPAN), cols]
            scores = mm_nt(q[pl.ds(row, BLOCK), cols], keys) * scaling
            seen = (distance >= 0) & (distance < window[h]) & (key_pos >= 0)
            scores = jnp.where(seen, scores, -1e30)
            expon = jnp.exp(scores - jnp.max(scores, axis=1, keepdims=True))
            expon = jnp.where(seen, expon, 0.0)
            probs = expon / jnp.sum(expon, axis=1, keepdims=True)
            p_all[h, b] = probs
            att[pl.ds(row, BLOCK), cols] = mm(probs.astype(BF), values).astype(BF)
        return carry

    lax.fori_loop(0, 3, forward, 0)

    grad.near_sides()
    grad.relay()
    inp.near_sides()
    grad.near_opposite()
    grad.across()
    inp.relay()
    inp.near_opposite()
    grad.far_sides()
    grad.far_opposite()
    grad.finish()
    loads["g"].wait()

    def produce(m, a, b):
        def quarter(xq):
            def chunk(j, carry):
                part[m, xq, j] = mm(a[j * 4 + xq], b[...]).astype(BF)
                return carry

            lax.fori_loop(0, 4, chunk, 0)

        tag = "w" + str(m)
        low, high = pl.ds(0, 2), pl.ds(2, 2)
        quarter(xo)
        send(tag + "a", part.at[m, xo, low], rel_l.at[m], x_right)
        send(tag + "b", part.at[m, xo, high], rel_r.at[m], x_left)
        quarter(xr)
        send(tag + "c", part.at[m, xr, high], rec_l.at[m, high], x_right)
        quarter(xl)
        send(tag + "d", part.at[m, xl, low], rec_r.at[m, low], x_left)
        quarter(x)

    def add_relays(m):
        tag = "w" + str(m)
        recv(tag + "a", rel_l.at[m])
        for j in range(2):
            total = part[m, xr, j].astype(F32) + rel_l[m, j].astype(F32)
            part[m, xr, j] = total.astype(BF)
        low, high = pl.ds(0, 2), pl.ds(2, 2)
        send(tag + "e", part.at[m, xr, low], rec_l.at[m, low], x_right)
        recv(tag + "b", rel_r.at[m])
        for j in range(2):
            total = part[m, xl, 2 + j].astype(F32) + rel_r[m, j].astype(F32)
            part[m, xl, 2 + j] = total.astype(BF)
        send(tag + "f", part.at[m, xl, high], rec_r.at[m, high], x_left)

    def sum_x(m):
        tag = "w" + str(m)
        low, high = pl.ds(0, 2), pl.ds(2, 2)
        recv(tag + "c", rec_l.at[m, high])
        recv(tag + "d", rec_r.at[m, low])
        recv(tag + "e", rec_l.at[m, low])
        recv(tag + "f", rec_r.at[m, high])

        def chunk(j, carry):
            total = part[m, x, j].astype(F32) + rec_l[m, j].astype(F32)
            zs[m, j] = (total + rec_r[m, j].astype(F32)).astype(BF)
            return carry

        lax.fori_loop(0, 4, chunk, 0)
        for d in (2, 1, 3):
            send(
                tag + "z" + str(d),
                zs.at[m, lax.rem(zl + d, 4)],
                zr.at[m, d - 1],
                z_low[d - 1],
            )

    def sum_z(m, out):
        for d in (1, 2, 3):
            recv("w" + str(m) + "z" + str(d), zr.at[m, d - 1])
        total = zs[m, zl].astype(F32)
        for d in range(3):
            total = total + zr[m, d].astype(F32)
        out[...] = total

    produce(0, g_all, att)

    loads["wo"].wait()
    head_grad = jnp.zeros((COLS, ROWS), F32)
    for i in range(8):
        head_grad = head_grad + mm(
            wo[:, pl.ds(640 * i, 640)], g_all[pl.ds(2 * i, 2)].reshape(640, ROWS)
        )
    hg[...] = jnp.transpose(head_grad).astype(BF)

    def backward(b, carry):
        row = pl.multiple_of(b * BLOCK, BLOCK)
        for h in range(2):
            cols = pl.ds(h * HD, HD)
            rows, span = pl.ds(row, BLOCK), pl.ds(row, SPAN)
            keys, values = kcat[span, cols], vcat[span, cols]
            grads = hg[rows, cols]
            probs = p_all[h, b]
            prob_grad = mm_nt(grads, values)
            row_term = jnp.sum(
                grads.astype(F32) * att[rows, cols].astype(F32), axis=1, keepdims=True
            )
            score_grad = (probs * (prob_grad - row_term)).astype(BF)
            dq[rows, cols] = (mm(score_grad, keys) * scaling).astype(BF)
            dk_acc[span, cols] += mm_tn(score_grad, q[rows, cols]) * scaling
            dv_acc[span, cols] += mm_tn(probs.astype(BF), grads)
        return carry

    lax.fori_loop(0, 3, backward, 0)
    halo_out[0] = dk_acc[pl.ds(PAD, WMAX)].astype(BF)
    halo_out[1] = dv_acc[pl.ds(PAD, WMAX)].astype(BF)
    send("hg", halo_out, halo_in, s_prev)

    inp.across()
    add_relays(0)
    inp.far_sides()
    inp.far_opposite()
    inp.finish()
    loads["x"].wait()
    produce(1, x_all, dq)

    recv("hg", halo_in)
    for acc, grads, i in ((dk_acc, dk, 0), (dv_acc, dv, 1)):
        own = pl.ds(PAD + WMAX, ROWS - WMAX)
        last = pl.ds(PAD + ROWS, WMAX)
        grads[pl.ds(0, ROWS - WMAX)] = acc[own].astype(BF)
        grads[pl.ds(ROWS - WMAX, WMAX)] = (acc[last] + halo_in[i].astype(F32)).astype(BF)

    sum_x(0)
    add_relays(1)
    produce(2, x_all, dk)

    for name in ("wq", "wk", "wv"):
        loads[name].wait()

    def ig_chunks(core):
        def chunk(j, carry):
            y_, zh_ = j // 2, lax.rem(j, 2)
            s = slot(zh_, y_, core)
            total = mm_nt(w_all[0, s], dq[...])
            total = total + mm_nt(w_all[1, s], dk[...])
            total = total + mm_nt(w_all[2, s], dv[...])
            igp[core, y_, zh_] = total.astype(BF)
            return carry

        lax.fori_loop(0, 8, chunk, 0)

    ig_chunks(1 - c)
    send("id", igp.at[1 - c], d2r, partner)
    ig_chunks(c)

    sum_x(1)
    add_relays(2)
    produce(3, x_all, dv)

    recv("id", d2r)

    def add_core(j, carry):
        y_, zh_ = j // 2, lax.rem(j, 2)
        total = igp[c, y_, zh_].astype(F32) + d2r[y_, zh_].astype(F32)
        igp[c, y_, zh_] = total.astype(BF)
        return carry

    lax.fori_loop(0, 8, add_core, 0)
    send("ia", igp.at[c, yo, 0], yrel.at[0], y_right)
    send("ib", igp.at[c, yo, 1], yrel.at[1], y_left)
    send("ic", igp.at[c, yr, 1], yrec.at[0, 1], y_right)
    send("ie", igp.at[c, yl, 0], yrec.at[1, 0], y_left)

    sum_x(2)
    recv("ia", yrel.at[0])
    igp[c, yr, 0] = (igp[c, yr, 0].astype(F32) + yrel[0].astype(F32)).astype(BF)
    send("if", igp.at[c, yr, 0], yrec.at[0, 0], y_right)
    recv("ib", yrel.at[1])
    igp[c, yl, 1] = (igp[c, yl, 1].astype(F32) + yrel[1].astype(F32)).astype(BF)
    send("ig", igp.at[c, yl, 1], yrec.at[1, 1], y_left)

    add_relays(3)

    recv("ic", yrec.at[0, 1])
    recv("ie", yrec.at[1, 0])
    recv("if", yrec.at[0, 0])
    recv("ig", yrec.at[1, 1])
    for i in range(2):
        total = igp[c, y, i].astype(F32) + yrec[0, i].astype(F32)
        zs_ig[i] = (total + yrec[1, i].astype(F32)).astype(BF)
    send("iq", zs_ig.at[1 - zh], zr_ig.at[0], z_far)

    sum_z(0, do_out)
    recv("iq", zr_ig.at[0])
    send("iz", zr_ig.at[0], zr_ig.at[1], z_next)
    sum_z(1, dq_out)

    sum_x(3)
    recv("iz", zr_ig.at[1])
    ig_out[...] = (zs_ig[zh].astype(F32) + zr_ig[1].astype(F32)).astype(BF)
    sum_z(2, dk_out)
    sum_z(3, dv_out)
    wire.finish()


def local(
    layer_input, query_rows, key_rows, value_rows, out_grad, window, w_query, w_key, w_value, w_out
):
    anywhere = pl.BlockSpec(memory_space=pl.ANY)
    vmem = pl.BlockSpec(memory_space=pltpu.VMEM)
    chunk = (SHARD, COLS)
    outs = pl.pallas_call(
        kernel,
        out_shape=(
            jax.ShapeDtypeStruct((SHARD, ROWS), BF),
            jax.ShapeDtypeStruct(chunk, F32),
            jax.ShapeDtypeStruct(chunk, F32),
            jax.ShapeDtypeStruct(chunk, F32),
            jax.ShapeDtypeStruct(chunk, F32),
        ),
        in_specs=[pl.BlockSpec(memory_space=pltpu.SMEM)] + [anywhere] * 9,
        out_specs=(vmem,) * 5,
        scratch_shapes=[
            pltpu.VMEM((16, SHARD, ROWS), BF),
            pltpu.VMEM((16, SHARD, ROWS), BF),
            pltpu.VMEM((2, SHARD, ROWS), BF),
            pltpu.VMEM((3, 16) + chunk, BF),
            pltpu.VMEM((COLS, 16 * SHARD), BF),
            pltpu.VMEM((ROWS, COLS), BF),
            pltpu.VMEM((KEYS, COLS), BF),
            pltpu.VMEM((KEYS, COLS), BF),
            pltpu.VMEM((2, 3, BLOCK, SPAN), F32),
            pltpu.VMEM((ROWS, COLS), BF),
            pltpu.VMEM((ROWS, COLS), BF),
            pltpu.VMEM((ROWS, COLS), BF),
            pltpu.VMEM((ROWS, COLS), BF),
            pltpu.VMEM((ROWS, COLS), BF),
            pltpu.VMEM((KEYS, COLS), F32),
            pltpu.VMEM((KEYS, COLS), F32),
            pltpu.VMEM((2, WMAX, COLS), BF),
            pltpu.VMEM((2, WMAX, COLS), BF),
            pltpu.VMEM((4, 4, 4) + chunk, BF),
            pltpu.VMEM((4, 2) + chunk, BF),
            pltpu.VMEM((4, 2) + chunk, BF),
            pltpu.VMEM((4, 4) + chunk, BF),
            pltpu.VMEM((4, 4) + chunk, BF),
            pltpu.VMEM((4, 4) + chunk, BF),
            pltpu.VMEM((4, 3) + chunk, BF),
            pltpu.VMEM((2, 4, 2, SHARD, ROWS), BF),
            pltpu.VMEM((4, 2, SHARD, ROWS), BF),
            pltpu.VMEM((2, SHARD, ROWS), BF),
            pltpu.VMEM((2, 2, SHARD, ROWS), BF),
            pltpu.VMEM((2, SHARD, ROWS), BF),
            pltpu.VMEM((2, SHARD, ROWS), BF),
            pltpu.SemaphoreType.DMA((SEMS,)),
            pltpu.SemaphoreType.DMA((SEMS,)),
            pltpu.SemaphoreType.DMA((9,)),
        ],
        compiler_params=pltpu.CompilerParams(
            collective_id=0, has_side_effects=True, vmem_limit_bytes=66_000_000
        ),
        name="layer_backward",
    )(
        window,
        layer_input.T,
        out_grad.T,
        query_rows,
        key_rows,
        value_rows,
        w_query.reshape(16, SHARD, COLS),
        w_key.reshape(16, SHARD, COLS),
        w_value.reshape(16, SHARD, COLS),
        w_out,
    )
    input_grad, query_grad, key_grad, value_grad, out_grad_t = outs
    return (input_grad.T, query_grad, key_grad, value_grad, out_grad_t.T)


def solution(mesh):
    in_specs = (
        P("section", "tensor"),
        P("section", "tensor"),
        P("section", "tensor"),
        P("section", "tensor"),
        P("section", "tensor"),
        P("tensor"),
        P(None, "tensor"),
        P(None, "tensor"),
        P(None, "tensor"),
        P("tensor", None),
    )
    out_specs = (
        P("section", "tensor"),
        P("section", "tensor"),
        P("section", "tensor"),
        P("section", "tensor"),
        P("tensor", "section"),
    )
    return jax.shard_map(local, mesh=mesh, in_specs=in_specs, out_specs=out_specs, check_vma=False)
```

```python
import math

import jax
import jax.numpy as jnp
from jax import lax
from jax.experimental import pallas as pl
from jax.experimental.pallas import tpu as pltpu
from jax.sharding import PartitionSpec as P

HD = 128
WMAX = 192
ROWS = 384
COLS = 256
SHARD = 320
PAD = 64
KEYS = PAD + WMAX + ROWS
BLOCK = 128
SPAN = 384
SEMS = 160
MESH = pl.DeviceIdType.MESH
BF = jnp.bfloat16
F32 = jnp.float32


def mm(a, b):
    return jnp.dot(a, b, preferred_element_type=F32)


def mm_nt(a, b):
    return lax.dot_general(a, b, (((1,), (1,)), ((), ())), preferred_element_type=F32)


def mm_tn(a, b):
    return lax.dot_general(a, b, (((0,), (0,)), ((), ())), preferred_element_type=F32)


class Wire:
    def __init__(self, send_sem, recv_sem, someone):
        self.send_sem, self.recv_sem, self.someone = send_sem, recv_sem, someone
        self.index = {}
        self.sent = []
        self.role = None

    def copy(self, name, src, dst, device):
        i = self.index.setdefault(name, len(self.index))
        assert i < SEMS
        return pltpu.make_async_remote_copy(
            src_ref=src,
            dst_ref=dst,
            send_sem=self.send_sem.at[i],
            recv_sem=self.recv_sem.at[i],
            device_id=device,
            device_id_type=MESH,
        )

    def send(self, name, src, dst, device, like=None):
        c = self.copy(name, src, dst, device)
        c.start()
        self.sent.append((self.role, c if like is None else (name, like)))

    def only(self, role, body):
        self.role = role
        pl.when(role)(body)
        self.role = None

    def recv(self, name, dst):
        self.copy(name, dst, dst, self.someone).wait_recv()

    def finish(self):
        for role, c in self.sent:
            if role is None:
                c.wait_send()
            else:

                def body(name=c[0], like=c[1]):
                    self.copy(name, like(), like(), self.someone).wait_send()

                pl.when(role)(body)


def kernel(
    window,
    x_in,
    g_in,
    q_in,
    k_in,
    v_in,
    wq_in,
    wk_in,
    wv_in,
    wo_in,
    ig_out,
    dq_out,
    dk_out,
    dv_out,
    do_out,
    g_all,
    xg,
    z_rel,
    w_all,
    wo,
    q,
    kcat,
    vcat,
    p_all,
    att,
    hg,
    d_all,
    dk_acc,
    dv_acc,
    halo_out,
    halo_in,
    part,
    rel_l,
    rel_r,
    rec_l,
    rec_r,
    pz,
    z1,
    zs,
    z2,
    igp,
    d2r,
    yrel,
    yrec,
    zs_ig,
    zr_ig,
    send_sem,
    recv_sem,
    load_sem,
    home_send,
    home_recv,
):
    section = lax.axis_index("section")
    tensor = lax.axis_index("tensor")
    zl, x = section // 4, lax.rem(section, 4)
    zh, y, c = tensor // 8, lax.rem(tensor // 2, 4), lax.rem(tensor, 2)
    zz = zh * 4 + zl
    way = 1 - 2 * c
    xr, xo, xl = lax.rem(x + 1, 4), lax.rem(x + 2, 4), lax.rem(x + 3, 4)
    yr, yo, yl = lax.rem(y + 1, 4), lax.rem(y + 2, 4), lax.rem(y + 3, 4)

    def at(x_=x, y_=y, zz_=zz, c_=c):
        return (lax.rem(zz_, 4) * 4 + x_, (zz_ // 4) * 8 + y_ * 2 + c_)

    def slot(zh_=zh, y_=y, c_=c):
        return zh_ * 8 + y_ * 2 + c_

    def zat(step, x_=x):
        return at(x_=x_, zz_=lax.rem(zz + step + 8, 8))

    partner = at(c_=1 - c)
    y_right, y_left = at(y_=yr), at(y_=yl)
    x_right, x_left = at(x_=xr), at(x_=xl)
    z_far = zat(3 * way)
    odd = lax.rem(zl, 2)
    z_one = ((zl + 1 - 2 * odd) * 4 + x, tensor)
    z_two = (lax.rem(zl + 2, 4) * 4 + x, tensor)
    s_next = (lax.rem(section + 1, 16), tensor)
    s_prev = (lax.rem(section + 15, 16), tensor)

    home = lax.rem(y, 2) * 2 + c
    to_home = lax.rem(home - x + 4, 4)
    on_core = c == lax.rem(x, 2)
    on_chip = lax.rem(y, 2) == x // 2
    holder = jnp.logical_and(on_core, on_chip)
    middle = jnp.logical_and(on_core, jnp.logical_not(on_chip))
    follower = jnp.logical_not(on_core)
    y_a = jnp.where(on_chip, y, yl)
    y_b = jnp.where(on_chip, yo, yr)

    loads = {}

    def load(name, src, dst):
        cp = pltpu.make_async_copy(src, dst, load_sem.at[len(loads)])
        loads[name] = cp
        cp.start()

    load("q", q_in, q)
    load("k", k_in, kcat.at[pl.ds(PAD + WMAX, ROWS)])
    load("v", v_in, vcat.at[pl.ds(PAD + WMAX, ROWS)])
    load("g", g_in, g_all.at[tensor])
    load("wo", wo_in, wo)
    load("wq", wq_in, w_all.at[0])
    load("wk", wk_in, w_all.at[1])
    load("wv", wv_in, w_all.at[2])
    own_x = pltpu.make_async_copy(x_in, xg.at[zh * 2 + y // 2, x], load_sem.at[len(loads)])
    pl.when(to_home == 0)(own_x.start)

    barrier = pltpu.get_barrier_semaphore()
    peers = [partner, y_right, y_left, x_right, x_left, at(x_=xo), s_next, s_prev]
    peers += [z_one, z_two, zat(3), zat(-3)]
    peers += [zat(step, x_) for step in (1, -1) for x_ in (x, xr, xo, xl)]
    for peer in peers:
        pl.semaphore_signal(barrier, inc=1, device_id=peer, device_id_type=MESH)
    pl.semaphore_wait(barrier, len(peers))

    wire = Wire(send_sem, recv_sem, partner)
    send, recv = wire.send, wire.recv

    class Gather:
        def __init__(self, tag, own, buf, rel):
            self.tag, self.own, self.buf, self.rel = tag, own, buf, rel

        def start(self):
            def own(i):
                return self.own.at[pl.ds(160 * i, 160)]

            for i in range(2):
                send(self.tag + "L" + str(i), own(i), self.half(tensor, i), y_right)
                send(self.tag + "R" + str(i), own(1 - i), self.half(tensor, 1 - i), y_left)
                send(self.tag + "Q" + str(i), own(i), self.rel.at[pl.ds(160 * i, 160)], z_far)
            send(self.tag + "P0", self.own, self.buf.at[tensor], partner)

        def half(self, s, i):
            return self.buf.at[s, pl.ds(160 * i, 160)]

        def sides(self, z, far, names):
            left, right = slot(far, yl), slot(far, yr)
            recv(self.tag + z + "L0", self.half(left, 0))
            send(self.tag + z + "OA", self.half(left, 0), self.half(left, 0), y_right)
            recv(self.tag + z + "R0", self.half(right, 1))
            send(self.tag + z + "OB", self.half(right, 1), self.half(right, 1), y_left)
            recv(self.tag + z + "L1", self.half(left, 1))
            send(self.tag + names[0], self.buf.at[left], self.buf.at[left], partner)
            recv(self.tag + z + "R1", self.half(right, 0))
            send(self.tag + names[1], self.buf.at[right], self.buf.at[right], partner)

        def opposite(self, z, far, name):
            here = slot(far, yo)
            recv(self.tag + z + "OA", self.half(here, 0))
            recv(self.tag + z + "OB", self.half(here, 1))
            send(self.tag + name, self.buf.at[here], self.buf.at[here], partner)

        def near_sides(self):
            self.sides("", zh, ("P1", "P2"))

        def near_opposite(self):
            self.opposite("", zh, "P3")

        def relay(self):
            source = lax.rem(zz - 3 * way + 8, 8)
            here = slot(source // 4)
            for i in range(2):
                piece = self.rel.at[pl.ds(160 * i, 160)]
                recv(self.tag + "Q" + str(i), piece)
                send(self.tag + "Z" + str(i), piece, self.half(here, i), zat(way))

        def across(self):
            here = slot(1 - zh)
            low, high = self.half(here, 0), self.half(here, 1)
            recv(self.tag + "Z0", low)
            send(self.tag + "ZL0", low, low, y_right)
            recv(self.tag + "Z1", high)
            send(self.tag + "ZR0", high, high, y_left)
            send(self.tag + "ZL1", high, high, y_right)
            send(self.tag + "ZR1", low, low, y_left)
            send(self.tag + "P4", self.buf.at[here], self.buf.at[here], partner)

        def far_sides(self):
            self.sides("Z", 1 - zh, ("P5", "P6"))

        def far_opposite(self):
            self.opposite("Z", 1 - zh, "P7")

        def finish(self, first):
            for i in range(first, first + 4):
                far = zh if i < 4 else 1 - zh
                where = (y, yl, yr, yo)[i % 4]
                recv(self.tag + "P" + str(i), self.buf.at[slot(far, where, 1 - c)])

    class Spread:
        def block(self, zh_, y_):
            return zh_ * 2 + y_ // 2

        def two(self):
            return xg.at[0, pl.ds(0, 2)]

        def four(self):
            return xg.at[0]

        def start(self):
            there = (zl * 4 + home, tensor)
            self.own = pltpu.make_async_remote_copy(
                src_ref=x_in,
                dst_ref=xg.at[self.block(zh, y), x],
                send_sem=home_send.at[0],
                recv_sem=home_recv.at[to_home],
                device_id=there,
                device_id_type=MESH,
            )
            pl.when(to_home != 0)(self.own.start)

        def start_far(self):
            send("xQ", x_in, z_rel.at[1], z_far)

        def relay(self):
            recv("xQ", z_rel.at[1])
            source = lax.rem(zz - 3 * way + 8, 8)
            self.far = pltpu.make_async_remote_copy(
                src_ref=z_rel.at[1],
                dst_ref=xg.at[self.block(source // 4, y), x],
                send_sem=home_send.at[1],
                recv_sem=home_recv.at[4 + to_home],
                device_id=zat(way, home),
                device_id_type=MESH,
            )
            self.far.start()

        def arrived(self, block, d, i):
            dst = xg.at[block, lax.rem(x - d + 4, 4)]
            pltpu.make_async_remote_copy(
                src_ref=dst,
                dst_ref=dst,
                send_sem=home_send.at[0],
                recv_sem=home_recv.at[i],
                device_id=partner,
                device_id_type=MESH,
            ).wait_recv()

        def spread(self, near, halves):
            tag = "xn" if near else "xf"
            far = zh if near else 1 - zh
            mine = self.block(far, y)

            def body():
                if 0 in halves:
                    if near:
                        own_x.wait()
                    else:
                        self.arrived(mine, 0, 4)
                    for d in (1, 2, 3):
                        self.arrived(mine, d, d if near else 4 + d)
                for i in halves:
                    half = xg.at[mine, pl.ds(2 * i, 2)]
                    send(tag + "L" + str(i), half, half, y_right, self.two)
                    send(tag + "R" + str(i), half, half, y_left, self.two)
                if 1 in halves:
                    send(tag + "A", xg.at[mine], xg.at[mine], partner, self.four)

            wire.only(holder, body)

        def forward(self, near):
            tag = "xn" if near else "xf"
            far = zh if near else 1 - zh
            left, right = self.block(far, yl), self.block(far, yr)

            def half(block, i):
                return xg.at[block, pl.ds(2 * i, 2)]

            def body():
                recv(tag + "L0", half(left, 0))
                send(tag + "OA", half(left, 0), half(left, 0), y_right, self.two)
                recv(tag + "R0", half(right, 0))
                recv(tag + "L1", half(left, 1))
                recv(tag + "R1", half(right, 1))
                send(tag + "OB", half(right, 1), half(right, 1), y_left, self.two)
                send(tag + "A", xg.at[left], xg.at[left], partner, self.four)
                send(tag + "B", xg.at[right], xg.at[right], partner, self.four)

            wire.only(middle, body)

        def opposite(self, near):
            tag = "xn" if near else "xf"
            far = zh if near else 1 - zh
            here = self.block(far, yo)

            def body():
                recv(tag + "OA", xg.at[here, pl.ds(0, 2)])
                recv(tag + "OB", xg.at[here, pl.ds(2, 2)])
                send(tag + "B", xg.at[here], xg.at[here], partner, self.four)

            wire.only(holder, body)

        def follow(self):
            def body():
                for tag, far in (("xn", zh), ("xf", 1 - zh)):
                    recv(tag + "A", xg.at[self.block(far, y_a)])
                    recv(tag + "B", xg.at[self.block(far, y_b)])

            wire.only(follower, body)

        def finish(self):
            pl.when(to_home != 0)(self.own.wait_send)
            self.far.wait_send()

    grad = Gather("g", g_in, g_all, z_rel.at[0])
    inp = Spread()
    halo_rows = pl.ds(ROWS - WMAX, WMAX)
    grad.start()
    send("hk", k_in.at[halo_rows], kcat.at[pl.ds(PAD, WMAX)], s_next)
    send("hv", v_in.at[halo_rows], vcat.at[pl.ds(PAD, WMAX)], s_next)
    inp.start()
    grad.near_sides()
    grad.relay()
    inp.start_far()
    grad.near_opposite()
    inp.spread(True, (0,))

    scaling = 1.0 / math.sqrt(HD)
    zero_rows = jnp.zeros((PAD, COLS), BF)
    kcat[pl.ds(0, PAD)] = zero_rows
    vcat[pl.ds(0, PAD)] = zero_rows
    dk_acc[...] = jnp.zeros_like(dk_acc)
    dv_acc[...] = jnp.zeros_like(dv_acc)
    loads["q"].wait()
    loads["k"].wait()
    loads["v"].wait()
    recv("hk", kcat.at[pl.ds(PAD, WMAX)])
    recv("hv", vcat.at[pl.ds(PAD, WMAX)])
    first = section * ROWS

    def forward(b, carry):
        row = pl.multiple_of(b * BLOCK, BLOCK)
        i = lax.broadcasted_iota(jnp.int32, (BLOCK, SPAN), 0)
        j = lax.broadcasted_iota(jnp.int32, (BLOCK, SPAN), 1)
        distance = i + (PAD + WMAX) - j
        key_pos = first - (PAD + WMAX) + row + j
        for h in range(2):
            cols = pl.ds(h * HD, HD)
            keys = kcat[pl.ds(row, SPAN), cols]
            values = vcat[pl.ds(row, SPAN), cols]
            scores = mm_nt(q[pl.ds(row, BLOCK), cols], keys) * scaling
            seen = (distance >= 0) & (distance < window[h]) & (key_pos >= 0)
            scores = jnp.where(seen, scores, -1e30)
            expon = jnp.exp(scores - jnp.max(scores, axis=1, keepdims=True))
            expon = jnp.where(seen, expon, 0.0)
            probs = expon / jnp.sum(expon, axis=1, keepdims=True)
            p_all[h, b] = probs
            att[pl.ds(row, BLOCK), cols] = mm(probs.astype(BF), values).astype(BF)
        return carry

    lax.fori_loop(0, 3, forward, 0)

    def out_start(i, tag):
        def quarter(xq):
            def chunk(side, carry):
                part[xq, side, i] = mm(g_all[(i * 2 + side) * 4 + xq], att[...]).astype(BF)
                return carry

            lax.fori_loop(0, 2, chunk, 0)

        quarter(xo)
        send(tag + "a", part.at[xo, 0, i], rel_l.at[i], x_right)
        send(tag + "b", part.at[xo, 1, i], rel_r.at[i], x_left)
        quarter(xr)
        quarter(xl)
        quarter(x)

    def out_rest(i, tag):
        send(tag + "c", part.at[xr, 1, i], rec_l.at[1, i], x_right)
        send(tag + "d", part.at[xl, 0, i], rec_r.at[0, i], x_left)

    def out_relay(i, tag):
        recv(tag + "a", rel_l.at[i])
        total = part[xr, 0, i].astype(F32) + rel_l[i].astype(F32)
        part[xr, 0, i] = total.astype(BF)
        send(tag + "e", part.at[xr, 0, i], rec_l.at[0, i], x_right)
        recv(tag + "b", rel_r.at[i])
        total = part[xl, 1, i].astype(F32) + rel_r[i].astype(F32)
        part[xl, 1, i] = total.astype(BF)
        send(tag + "f", part.at[xl, 1, i], rec_r.at[1, i], x_left)

    def out_sum(i, tag):
        recv(tag + "c", rec_l.at[1, i])
        recv(tag + "d", rec_r.at[0, i])
        recv(tag + "e", rec_l.at[0, i])
        recv(tag + "f", rec_r.at[1, i])

        def chunk(side, carry):
            total = part[x, side, i].astype(F32) + rec_l[side, i].astype(F32)
            pz[0, side, i] = (total + rec_r[side, i].astype(F32)).astype(BF)
            return carry

        lax.fori_loop(0, 2, chunk, 0)
        send("z" + tag, pz.at[0, 1 - odd, i], z1.at[0, i], z_one)

    def share(m):
        mine = d_all.at[m - 1, x]
        send("aL" + str(m), mine, mine, x_right)
        send("aR" + str(m), mine, mine, x_left)

    def share_on(m):
        left, right = d_all.at[m - 1, xl], d_all.at[m - 1, xr]
        recv("aL" + str(m), left)
        half = d_all.at[m - 1, xl, pl.ds(0, 192)]
        send("aA" + str(m), half, half, x_right)
        recv("aR" + str(m), right)
        half = d_all.at[m - 1, xr, pl.ds(192, 192)]
        send("aB" + str(m), half, half, x_left)

    def produce(m):
        recv("aA" + str(m), d_all.at[m - 1, xo, pl.ds(0, 192)])
        recv("aB" + str(m), d_all.at[m - 1, xo, pl.ds(192, 192)])

        def chunks(side):
            def chunk(i, carry):
                total = mm(xg[i * 2 + side, 0], d_all[m - 1, 0])
                for r in range(1, 4):
                    total = total + mm(xg[i * 2 + side, r], d_all[m - 1, r])
                pz[m, side, i] = total.astype(BF)
                return carry

            lax.fori_loop(0, 2, chunk, 0)

        chunks(1 - odd)
        send("z1_" + str(m), pz.at[m, 1 - odd], z1.at[m], z_one)
        chunks(odd)

    def halve(m):
        if m:
            recv("z1_" + str(m), z1.at[m])
        else:
            recv("zn", z1.at[0, zh])
            recv("zf", z1.at[0, 1 - zh])
        other = 1 - zl // 2
        zs[m] = (pz[m, odd, other].astype(F32) + z1[m, other].astype(F32)).astype(BF)
        send("z2_" + str(m), zs.at[m], z2.at[m], z_two)

    def sum_z(m, out):
        recv("z2_" + str(m), z2.at[m])
        total = pz[m, odd, zl // 2].astype(F32) + z1[m, zl // 2].astype(F32)
        out[...] = total + z2[m].astype(F32)

    grad.finish(0)
    loads["g"].wait()
    grad.across()
    out_start(zh, "n")
    out_rest(zh, "n")
    grad.far_sides()
    inp.spread(True, (1,))
    inp.relay()
    out_relay(zh, "n")
    grad.far_opposite()
    grad.finish(4)

    loads["wo"].wait()
    head_grad = jnp.zeros((COLS, ROWS), F32)
    for i in range(8):
        head_grad = head_grad + mm(
            wo[:, pl.ds(640 * i, 640)], g_all[pl.ds(2 * i, 2)].reshape(640, ROWS)
        )
    hg[...] = jnp.transpose(head_grad).astype(BF)

    def backward(b, carry):
        row = pl.multiple_of(b * BLOCK, BLOCK)
        for h in range(2):
            cols = pl.ds(h * HD, HD)
            rows, span = pl.ds(row, BLOCK), pl.ds(row, SPAN)
            keys, values = kcat[span, cols], vcat[span, cols]
            grads = hg[rows, cols]
            probs = p_all[h, b]
            prob_grad = mm_nt(grads, values)
            row_term = jnp.sum(
                grads.astype(F32) * att[rows, cols].astype(F32), axis=1, keepdims=True
            )
            score_grad = (probs * (prob_grad - row_term)).astype(BF)
            d_all[0, x, rows, cols] = (mm(score_grad, keys) * scaling).astype(BF)
            dk_acc[span, cols] += mm_tn(score_grad, q[rows, cols]) * scaling
            dv_acc[span, cols] += mm_tn(probs.astype(BF), grads)
        return carry

    lax.fori_loop(0, 3, backward, 0)
    halo_out[0] = dk_acc[pl.ds(PAD, WMAX)].astype(BF)
    halo_out[1] = dv_acc[pl.ds(PAD, WMAX)].astype(BF)

    share(1)
    send("hg", halo_out, halo_in, s_prev)
    inp.spread(False, (0, 1))
    out_start(1 - zh, "f")
    inp.forward(True)
    out_sum(zh, "n")
    share_on(1)
    inp.opposite(True)
    recv("hg", halo_in)
    for acc, i in ((dk_acc, 0), (dv_acc, 1)):
        own = pl.ds(PAD + WMAX, ROWS - WMAX)
        last = pl.ds(PAD + ROWS, WMAX)
        d_all[1 + i, x, pl.ds(0, ROWS - WMAX)] = acc[own].astype(BF)
        d_all[1 + i, x, pl.ds(ROWS - WMAX, WMAX)] = (acc[last] + halo_in[i].astype(F32)).astype(BF)

    share(2)
    share(3)
    out_rest(1 - zh, "f")

    for name in ("wq", "wk", "wv"):
        loads[name].wait()

    def ig_chunks(core):
        def chunk(j, carry):
            y_, zh_ = j // 2, lax.rem(j, 2)
            s = slot(zh_, y_, core)
            total = mm_nt(w_all[0, s], d_all[0, x])
            total = total + mm_nt(w_all[1, s], d_all[1, x])
            total = total + mm_nt(w_all[2, s], d_all[2, x])
            igp[core, y_, zh_] = total.astype(BF)
            return carry

        lax.fori_loop(0, 8, chunk, 0)

    ig_chunks(1 - c)
    send("id", igp.at[1 - c], d2r, partner)
    inp.forward(False)
    ig_chunks(c)
    inp.opposite(False)
    inp.follow()
    produce(1)
    recv("id", d2r)

    def add_core(j, carry):
        y_, zh_ = j // 2, lax.rem(j, 2)
        total = igp[c, y_, zh_].astype(F32) + d2r[y_, zh_].astype(F32)
        igp[c, y_, zh_] = total.astype(BF)
        return carry

    lax.fori_loop(0, 8, add_core, 0)
    send("ia", igp.at[c, yo, 0], yrel.at[0], y_right)
    send("ib", igp.at[c, yo, 1], yrel.at[1], y_left)
    send("ic", igp.at[c, yr, 1], yrec.at[0, 1], y_right)
    send("ie", igp.at[c, yl, 0], yrec.at[1, 0], y_left)

    share_on(2)
    out_relay(1 - zh, "f")
    produce(2)
    share_on(3)
    recv("ia", yrel.at[0])
    igp[c, yr, 0] = (igp[c, yr, 0].astype(F32) + yrel[0].astype(F32)).astype(BF)
    send("if", igp.at[c, yr, 0], yrec.at[0, 0], y_right)
    recv("ib", yrel.at[1])
    igp[c, yl, 1] = (igp[c, yl, 1].astype(F32) + yrel[1].astype(F32)).astype(BF)
    send("ig", igp.at[c, yl, 1], yrec.at[1, 1], y_left)

    produce(3)
    halve(1)
    out_sum(1 - zh, "f")
    recv("ic", yrec.at[0, 1])
    recv("ie", yrec.at[1, 0])
    recv("if", yrec.at[0, 0])
    recv("ig", yrec.at[1, 1])
    for i in range(2):
        total = igp[c, y, i].astype(F32) + yrec[0, i].astype(F32)
        zs_ig[i] = (total + yrec[1, i].astype(F32)).astype(BF)
    send("iq", zs_ig.at[1 - zh], zr_ig.at[0], z_far)

    halve(2)
    halve(0)
    halve(3)
    sum_z(0, do_out)
    recv("iq", zr_ig.at[0])
    send("iz", zr_ig.at[0], zr_ig.at[1], zat(way))
    sum_z(1, dq_out)
    sum_z(2, dk_out)
    sum_z(3, dv_out)
    recv("iz", zr_ig.at[1])
    ig_out[...] = (zs_ig[zh].astype(F32) + zr_ig[1].astype(F32)).astype(BF)
    inp.finish()
    wire.finish()


def leave(*refs):
    sources, targets, held = refs[:5], refs[5:10], refs[10:15]
    into, out = refs[15:]
    first = [
        pltpu.make_async_copy(s, h, into.at[i]) for i, (s, h) in enumerate(zip(sources, held))
    ]
    second = [
        pltpu.make_async_copy(h, t, out.at[i]) for i, (h, t) in enumerate(zip(held, targets))
    ]
    for cp in first:
        cp.start()
    for a, b in zip(first, second):
        a.wait()
        b.start()
    for cp in second:
        cp.wait()


def local(
    layer_input, query_rows, key_rows, value_rows, out_grad, window, w_query, w_key, w_value, w_out
):
    anywhere = pl.BlockSpec(memory_space=pl.ANY)
    vmem = pl.BlockSpec(memory_space=pltpu.VMEM)
    chunk = (SHARD, COLS)
    outs = pl.pallas_call(
        kernel,
        out_shape=(
            jax.ShapeDtypeStruct((SHARD, ROWS), BF),
            jax.ShapeDtypeStruct(chunk, F32),
            jax.ShapeDtypeStruct(chunk, F32),
            jax.ShapeDtypeStruct(chunk, F32),
            jax.ShapeDtypeStruct(chunk, F32),
        ),
        in_specs=[pl.BlockSpec(memory_space=pltpu.SMEM)] + [anywhere] * 9,
        out_specs=(vmem,) * 5,
        scratch_shapes=[
            pltpu.VMEM((16, SHARD, ROWS), BF),
            pltpu.VMEM((4, 4, SHARD, ROWS), BF),
            pltpu.VMEM((2, SHARD, ROWS), BF),
            pltpu.VMEM((3, 16) + chunk, BF),
            pltpu.VMEM((COLS, 16 * SHARD), BF),
            pltpu.VMEM((ROWS, COLS), BF),
            pltpu.VMEM((KEYS, COLS), BF),
            pltpu.VMEM((KEYS, COLS), BF),
            pltpu.VMEM((2, 3, BLOCK, SPAN), F32),
            pltpu.VMEM((ROWS, COLS), BF),
            pltpu.VMEM((ROWS, COLS), BF),
            pltpu.VMEM((3, 4, ROWS, COLS), BF),
            pltpu.VMEM((KEYS, COLS), F32),
            pltpu.VMEM((KEYS, COLS), F32),
            pltpu.VMEM((2, WMAX, COLS), BF),
            pltpu.VMEM((2, WMAX, COLS), BF),
            pltpu.VMEM((4, 2, 2) + chunk, BF),
            pltpu.VMEM((2,) + chunk, BF),
            pltpu.VMEM((2,) + chunk, BF),
            pltpu.VMEM((2, 2) + chunk, BF),
            pltpu.VMEM((2, 2) + chunk, BF),
            pltpu.VMEM((4, 2, 2) + chunk, BF),
            pltpu.VMEM((4, 2) + chunk, BF),
            pltpu.VMEM((4,) + chunk, BF),
            pltpu.VMEM((4,) + chunk, BF),
            pltpu.VMEM((2, 4, 2, SHARD, ROWS), BF),
            pltpu.VMEM((4, 2, SHARD, ROWS), BF),
            pltpu.VMEM((2, SHARD, ROWS), BF),
            pltpu.VMEM((2, 2, SHARD, ROWS), BF),
            pltpu.VMEM((2, SHARD, ROWS), BF),
            pltpu.VMEM((2, SHARD, ROWS), BF),
            pltpu.SemaphoreType.DMA((SEMS,)),
            pltpu.SemaphoreType.DMA((SEMS,)),
            pltpu.SemaphoreType.DMA((9,)),
            pltpu.SemaphoreType.DMA((2,)),
            pltpu.SemaphoreType.DMA((8,)),
        ],
        compiler_params=pltpu.CompilerParams(
            collective_id=0, has_side_effects=True, vmem_limit_bytes=66_000_000
        ),
        name="layer_backward",
    )(
        window,
        layer_input.T,
        out_grad.T,
        query_rows,
        key_rows,
        value_rows,
        w_query.reshape(16, SHARD, COLS),
        w_key.reshape(16, SHARD, COLS),
        w_value.reshape(16, SHARD, COLS),
        w_out,
    )
    shapes = tuple(jax.ShapeDtypeStruct(o.shape, o.dtype) for o in outs)
    outs = pl.pallas_call(
        leave,
        out_shape=shapes,
        in_specs=[anywhere] * 5,
        out_specs=(anywhere,) * 5,
        scratch_shapes=[pltpu.VMEM(o.shape, o.dtype) for o in outs]
        + [pltpu.SemaphoreType.DMA((5,)), pltpu.SemaphoreType.DMA((5,))],
        name="leave",
    )(*outs)
    input_grad, query_grad, key_grad, value_grad, out_grad_t = outs
    return (input_grad.T, query_grad, key_grad, value_grad, out_grad_t.T)


def solution(mesh):
    in_specs = (
        P("section", "tensor"),
        P("section", "tensor"),
        P("section", "tensor"),
        P("section", "tensor"),
        P("section", "tensor"),
        P("tensor"),
        P(None, "tensor"),
        P(None, "tensor"),
        P(None, "tensor"),
        P("tensor", None),
    )
    out_specs = (
        P("section", "tensor"),
        P("section", "tensor"),
        P("section", "tensor"),
        P("section", "tensor"),
        P("tensor", "section"),
    )
    return jax.shard_map(local, mesh=mesh, in_specs=in_specs, out_specs=out_specs, check_vma=False)
```

```python
import math

import jax
import jax.numpy as jnp
from jax import lax
from jax.experimental import pallas as pl
from jax.experimental.pallas import tpu as pltpu
from jax.sharding import PartitionSpec as P

HD = 128
WMAX = 192
ROWS = 384
COLS = 256
SHARD = 320
PAD = 64
KEYS = PAD + WMAX + ROWS
BLOCK = 128
SPAN = 384
SEMS = 160
MESH = pl.DeviceIdType.MESH
BF = jnp.bfloat16
F32 = jnp.float32


def mm(a, b):
    return jnp.dot(a, b, preferred_element_type=F32)


def mm_nt(a, b):
    return lax.dot_general(a, b, (((1,), (1,)), ((), ())), preferred_element_type=F32)


def mm_tn(a, b):
    return lax.dot_general(a, b, (((0,), (0,)), ((), ())), preferred_element_type=F32)


class Wire:
    def __init__(self, send_sem, recv_sem, someone):
        self.send_sem, self.recv_sem, self.someone = send_sem, recv_sem, someone
        self.index = {}
        self.sent = []
        self.role = None

    def copy(self, name, src, dst, device):
        i = self.index.setdefault(name, len(self.index))
        assert i < SEMS
        return pltpu.make_async_remote_copy(
            src_ref=src,
            dst_ref=dst,
            send_sem=self.send_sem.at[i],
            recv_sem=self.recv_sem.at[i],
            device_id=device,
            device_id_type=MESH,
        )

    def send(self, name, src, dst, device, like=None):
        c = self.copy(name, src, dst, device)
        c.start()
        self.sent.append((self.role, c if like is None else (name, like)))

    def only(self, role, body):
        self.role = role
        pl.when(role)(body)
        self.role = None

    def recv(self, name, dst):
        self.copy(name, dst, dst, self.someone).wait_recv()

    def finish(self):
        for role, c in self.sent:
            if role is None:
                c.wait_send()
            else:

                def body(name=c[0], like=c[1]):
                    self.copy(name, like(), like(), self.someone).wait_send()

                pl.when(role)(body)


def kernel(
    window,
    x_in,
    g_in,
    q_in,
    k_in,
    v_in,
    wq_in,
    wk_in,
    wv_in,
    wo_in,
    ig_out,
    dq_out,
    dk_out,
    dv_out,
    do_out,
    g_all,
    xg,
    z_rel,
    w_all,
    wo,
    q,
    kcat,
    vcat,
    p_all,
    att,
    hg,
    hg_acc,
    d_all,
    dk_acc,
    dv_acc,
    halo_out,
    halo_in,
    part,
    rel_l,
    rel_r,
    rec_l,
    rec_r,
    pz,
    z1,
    zs,
    z2,
    igp,
    d2r,
    yrel,
    yrec,
    zs_ig,
    zr_ig,
    send_sem,
    recv_sem,
    load_sem,
    home_send,
    home_recv,
):
    section = lax.axis_index("section")
    tensor = lax.axis_index("tensor")
    zl, x = section // 4, lax.rem(section, 4)
    zh, y, c = tensor // 8, lax.rem(tensor // 2, 4), lax.rem(tensor, 2)
    zz = zh * 4 + zl
    way = 1 - 2 * c
    xr, xo, xl = lax.rem(x + 1, 4), lax.rem(x + 2, 4), lax.rem(x + 3, 4)
    yr, yo, yl = lax.rem(y + 1, 4), lax.rem(y + 2, 4), lax.rem(y + 3, 4)

    def at(x_=x, y_=y, zz_=zz, c_=c):
        return (lax.rem(zz_, 4) * 4 + x_, (zz_ // 4) * 8 + y_ * 2 + c_)

    def slot(zh_=zh, y_=y, c_=c):
        return zh_ * 8 + y_ * 2 + c_

    def zat(step, x_=x):
        return at(x_=x_, zz_=lax.rem(zz + step + 8, 8))

    partner = at(c_=1 - c)
    y_right, y_left = at(y_=yr), at(y_=yl)
    x_right, x_left = at(x_=xr), at(x_=xl)
    z_far = zat(3 * way)
    odd = lax.rem(zl, 2)
    z_one = ((zl + 1 - 2 * odd) * 4 + x, tensor)
    z_two = (lax.rem(zl + 2, 4) * 4 + x, tensor)
    s_next = (lax.rem(section + 1, 16), tensor)
    s_prev = (lax.rem(section + 15, 16), tensor)

    home = lax.rem(y, 2) * 2 + c
    to_home = lax.rem(home - x + 4, 4)
    on_core = c == lax.rem(x, 2)
    on_chip = lax.rem(y, 2) == x // 2
    holder = jnp.logical_and(on_core, on_chip)
    middle = jnp.logical_and(on_core, jnp.logical_not(on_chip))
    follower = jnp.logical_not(on_core)
    y_a = jnp.where(on_chip, y, yl)
    y_b = jnp.where(on_chip, yo, yr)

    loads = {}

    def load(name, src, dst):
        cp = pltpu.make_async_copy(src, dst, load_sem.at[len(loads)])
        loads[name] = cp
        cp.start()

    load("q", q_in, q)
    load("k", k_in, kcat.at[pl.ds(PAD + WMAX, ROWS)])
    load("v", v_in, vcat.at[pl.ds(PAD + WMAX, ROWS)])
    load("g", g_in, g_all.at[tensor])
    load("wo", wo_in, wo)
    load("wq", wq_in, w_all.at[0])
    load("wk", wk_in, w_all.at[1])
    load("wv", wv_in, w_all.at[2])
    own_x = pltpu.make_async_copy(x_in, xg.at[zh * 2 + y // 2, x], load_sem.at[len(loads)])
    pl.when(to_home == 0)(own_x.start)

    barrier = pltpu.get_barrier_semaphore()
    peers = [partner, y_right, y_left, x_right, x_left, at(x_=xo), s_next, s_prev]
    peers += [z_one, z_two, zat(3), zat(-3)]
    peers += [zat(step, x_) for step in (1, -1) for x_ in (x, xr, xo, xl)]
    for peer in peers:
        pl.semaphore_signal(barrier, inc=1, device_id=peer, device_id_type=MESH)
    pl.semaphore_wait(barrier, len(peers))

    wire = Wire(send_sem, recv_sem, partner)
    send, recv = wire.send, wire.recv

    class Gather:
        def __init__(self, tag, own, buf, rel):
            self.tag, self.own, self.buf, self.rel = tag, own, buf, rel

        def start(self):
            def own(i):
                return self.own.at[pl.ds(160 * i, 160)]

            for i in range(2):
                send(self.tag + "L" + str(i), own(i), self.half(tensor, i), y_right)
                send(self.tag + "R" + str(i), own(1 - i), self.half(tensor, 1 - i), y_left)
                send(self.tag + "Q" + str(i), own(i), self.rel.at[pl.ds(160 * i, 160)], z_far)
            send(self.tag + "P0", self.own, self.buf.at[tensor], partner)

        def half(self, s, i):
            return self.buf.at[s, pl.ds(160 * i, 160)]

        def sides(self, z, far, names, steps):
            left, right = slot(far, yl), slot(far, yr)
            if 0 in steps:
                recv(self.tag + z + "L0", self.half(left, 0))
                send(self.tag + z + "OA", self.half(left, 0), self.half(left, 0), y_right)
                recv(self.tag + z + "R0", self.half(right, 1))
                send(self.tag + z + "OB", self.half(right, 1), self.half(right, 1), y_left)
            if 1 in steps:
                recv(self.tag + z + "L1", self.half(left, 1))
                send(self.tag + names[0], self.buf.at[left], self.buf.at[left], partner)
                recv(self.tag + z + "R1", self.half(right, 0))
                send(self.tag + names[1], self.buf.at[right], self.buf.at[right], partner)

        def opposite(self, z, far, name):
            here = slot(far, yo)
            recv(self.tag + z + "OA", self.half(here, 0))
            recv(self.tag + z + "OB", self.half(here, 1))
            send(self.tag + name, self.buf.at[here], self.buf.at[here], partner)

        def near_sides(self):
            self.sides("", zh, ("P1", "P2"), (0, 1))

        def near_opposite(self):
            self.opposite("", zh, "P3")

        def relay(self):
            source = lax.rem(zz - 3 * way + 8, 8)
            here = slot(source // 4)
            for i in range(2):
                piece = self.rel.at[pl.ds(160 * i, 160)]
                recv(self.tag + "Q" + str(i), piece)
                send(self.tag + "Z" + str(i), piece, self.half(here, i), zat(way))

        def across(self):
            here = slot(1 - zh)
            low, high = self.half(here, 0), self.half(here, 1)
            recv(self.tag + "Z0", low)
            send(self.tag + "ZL0", low, low, y_right)
            recv(self.tag + "Z1", high)
            send(self.tag + "ZR0", high, high, y_left)
            send(self.tag + "ZL1", high, high, y_right)
            send(self.tag + "ZR1", low, low, y_left)
            send(self.tag + "P4", self.buf.at[here], self.buf.at[here], partner)

        def far_sides(self, step):
            self.sides("Z", 1 - zh, ("P5", "P6"), (step,))

        def far_opposite(self):
            self.opposite("Z", 1 - zh, "P7")

        def finish(self, first):
            for i in range(first, first + 4):
                far = zh if i < 4 else 1 - zh
                where = (y, yl, yr, yo)[i % 4]
                recv(self.tag + "P" + str(i), self.buf.at[slot(far, where, 1 - c)])

    class Spread:
        def block(self, zh_, y_):
            return zh_ * 2 + y_ // 2

        def two(self):
            return xg.at[0, pl.ds(0, 2)]

        def four(self):
            return xg.at[0]

        def start(self):
            there = (zl * 4 + home, tensor)
            self.own = pltpu.make_async_remote_copy(
                src_ref=x_in,
                dst_ref=xg.at[self.block(zh, y), x],
                send_sem=home_send.at[0],
                recv_sem=home_recv.at[to_home],
                device_id=there,
                device_id_type=MESH,
            )
            pl.when(to_home != 0)(self.own.start)

        def start_far(self):
            send("xQ", x_in, z_rel.at[1], z_far)

        def relay(self):
            recv("xQ", z_rel.at[1])
            source = lax.rem(zz - 3 * way + 8, 8)
            self.far = pltpu.make_async_remote_copy(
                src_ref=z_rel.at[1],
                dst_ref=xg.at[self.block(source // 4, y), x],
                send_sem=home_send.at[1],
                recv_sem=home_recv.at[4 + to_home],
                device_id=zat(way, home),
                device_id_type=MESH,
            )
            self.far.start()

        def arrived(self, block, d, i):
            dst = xg.at[block, lax.rem(x - d + 4, 4)]
            pltpu.make_async_remote_copy(
                src_ref=dst,
                dst_ref=dst,
                send_sem=home_send.at[0],
                recv_sem=home_recv.at[i],
                device_id=partner,
                device_id_type=MESH,
            ).wait_recv()

        def spread(self, near, halves):
            tag = "xn" if near else "xf"
            far = zh if near else 1 - zh
            mine = self.block(far, y)

            def body():
                if 0 in halves:
                    if near:
                        own_x.wait()
                    else:
                        self.arrived(mine, 0, 4)
                    for d in (1, 2, 3):
                        self.arrived(mine, d, d if near else 4 + d)
                for i in halves:
                    half = xg.at[mine, pl.ds(2 * i, 2)]
                    send(tag + "L" + str(i), half, half, y_right, self.two)
                    half = xg.at[mine, pl.ds(2 - 2 * i, 2)]
                    send(tag + "R" + str(i), half, half, y_left, self.two)
                if 1 in halves:
                    send(tag + "A", xg.at[mine], xg.at[mine], partner, self.four)

            wire.only(holder, body)

        def forward(self, near, first):
            tag = "xn" if near else "xf"
            far = zh if near else 1 - zh
            left, right = self.block(far, yl), self.block(far, yr)

            def half(block, i):
                return xg.at[block, pl.ds(2 * i, 2)]

            def body():
                if first:
                    recv(tag + "L0", half(left, 0))
                    send(tag + "OA", half(left, 0), half(left, 0), y_right, self.two)
                    recv(tag + "R0", half(right, 1))
                    send(tag + "OB", half(right, 1), half(right, 1), y_left, self.two)
                else:
                    recv(tag + "L1", half(left, 1))
                    send(tag + "A", xg.at[left], xg.at[left], partner, self.four)
                    recv(tag + "R1", half(right, 0))
                    send(tag + "B", xg.at[right], xg.at[right], partner, self.four)

            wire.only(middle, body)

        def opposite(self, near):
            tag = "xn" if near else "xf"
            far = zh if near else 1 - zh
            here = self.block(far, yo)

            def body():
                recv(tag + "OA", xg.at[here, pl.ds(0, 2)])
                recv(tag + "OB", xg.at[here, pl.ds(2, 2)])
                send(tag + "B", xg.at[here], xg.at[here], partner, self.four)

            wire.only(holder, body)

        def follow(self):
            def body():
                for tag, far in (("xn", zh), ("xf", 1 - zh)):
                    recv(tag + "A", xg.at[self.block(far, y_a)])
                    recv(tag + "B", xg.at[self.block(far, y_b)])

            wire.only(follower, body)

        def finish(self):
            pl.when(to_home != 0)(self.own.wait_send)
            self.far.wait_send()

    grad = Gather("g", g_in, g_all, z_rel.at[0])
    inp = Spread()
    halo_rows = pl.ds(ROWS - WMAX, WMAX)
    grad.start()
    send("hk", k_in.at[halo_rows], kcat.at[pl.ds(PAD, WMAX)], s_next)
    send("hv", v_in.at[halo_rows], vcat.at[pl.ds(PAD, WMAX)], s_next)
    inp.start()
    grad.near_sides()
    grad.relay()
    inp.start_far()
    grad.near_opposite()
    inp.spread(True, (0,))

    scaling = 1.0 / math.sqrt(HD)
    zero_rows = jnp.zeros((PAD, COLS), BF)
    kcat[pl.ds(0, PAD)] = zero_rows
    vcat[pl.ds(0, PAD)] = zero_rows
    dk_acc[...] = jnp.zeros_like(dk_acc)
    dv_acc[...] = jnp.zeros_like(dv_acc)
    loads["q"].wait()
    loads["k"].wait()
    loads["v"].wait()
    recv("hk", kcat.at[pl.ds(PAD, WMAX)])
    recv("hv", vcat.at[pl.ds(PAD, WMAX)])
    first = section * ROWS

    def forward(b, carry):
        row = pl.multiple_of(b * BLOCK, BLOCK)
        i = lax.broadcasted_iota(jnp.int32, (BLOCK, SPAN), 0)
        j = lax.broadcasted_iota(jnp.int32, (BLOCK, SPAN), 1)
        distance = i + (PAD + WMAX) - j
        key_pos = first - (PAD + WMAX) + row + j
        for h in range(2):
            cols = pl.ds(h * HD, HD)
            keys = kcat[pl.ds(row, SPAN), cols]
            values = vcat[pl.ds(row, SPAN), cols]
            scores = mm_nt(q[pl.ds(row, BLOCK), cols], keys) * scaling
            seen = (distance >= 0) & (distance < window[h]) & (key_pos >= 0)
            scores = jnp.where(seen, scores, -1e30)
            expon = jnp.exp(scores - jnp.max(scores, axis=1, keepdims=True))
            expon = jnp.where(seen, expon, 0.0)
            probs = expon / jnp.sum(expon, axis=1, keepdims=True)
            p_all[h, b] = probs
            att[pl.ds(row, BLOCK), cols] = mm(probs.astype(BF), values).astype(BF)
        return carry

    lax.fori_loop(0, 3, forward, 0)

    def out_start(i, tag):
        def quarter(xq):
            def chunk(side, carry):
                part[xq, side, i] = mm(g_all[(i * 2 + side) * 4 + xq], att[...]).astype(BF)
                return carry

            lax.fori_loop(0, 2, chunk, 0)

        quarter(xo)
        send(tag + "a", part.at[xo, 0, i], rel_l.at[i], x_right)
        quarter(xr)
        quarter(xl)
        quarter(x)

    def out_rest(i, tag):
        send(tag + "b", part.at[xo, 1, i], rel_r.at[i], x_left)
        send(tag + "c", part.at[xr, 1, i], rec_l.at[1, i], x_right)
        send(tag + "d", part.at[xl, 0, i], rec_r.at[0, i], x_left)

    def out_relay(i, tag):
        recv(tag + "a", rel_l.at[i])
        total = part[xr, 0, i].astype(F32) + rel_l[i].astype(F32)
        part[xr, 0, i] = total.astype(BF)
        send(tag + "e", part.at[xr, 0, i], rec_l.at[0, i], x_right)
        recv(tag + "b", rel_r.at[i])
        total = part[xl, 1, i].astype(F32) + rel_r[i].astype(F32)
        part[xl, 1, i] = total.astype(BF)
        send(tag + "f", part.at[xl, 1, i], rec_r.at[1, i], x_left)

    def out_sum(i, tag):
        recv(tag + "c", rec_l.at[1, i])
        recv(tag + "d", rec_r.at[0, i])
        recv(tag + "e", rec_l.at[0, i])
        recv(tag + "f", rec_r.at[1, i])

        def chunk(side, carry):
            total = part[x, side, i].astype(F32) + rec_l[side, i].astype(F32)
            pz[0, side, i] = (total + rec_r[side, i].astype(F32)).astype(BF)
            return carry

        lax.fori_loop(0, 2, chunk, 0)
        send("z" + tag, pz.at[0, 1 - odd, i], z1.at[0, i], z_one)

    def share(m):
        mine = d_all.at[m - 1, x]
        send("aL" + str(m), mine, mine, x_right)
        send("aR" + str(m), mine, mine, x_left)

    def share_on(m):
        left, right = d_all.at[m - 1, xl], d_all.at[m - 1, xr]
        recv("aL" + str(m), left)
        half = d_all.at[m - 1, xl, pl.ds(0, 192)]
        send("aA" + str(m), half, half, x_right)
        recv("aR" + str(m), right)
        half = d_all.at[m - 1, xr, pl.ds(192, 192)]
        send("aB" + str(m), half, half, x_left)

    def produce(m):
        recv("aA" + str(m), d_all.at[m - 1, xo, pl.ds(0, 192)])
        recv("aB" + str(m), d_all.at[m - 1, xo, pl.ds(192, 192)])

        def chunks(side):
            def chunk(i, carry):
                total = mm(xg[i * 2 + side, 0], d_all[m - 1, 0])
                for r in range(1, 4):
                    total = total + mm(xg[i * 2 + side, r], d_all[m - 1, r])
                pz[m, side, i] = total.astype(BF)
                return carry

            lax.fori_loop(0, 2, chunk, 0)

        chunks(1 - odd)
        send("z1_" + str(m), pz.at[m, 1 - odd], z1.at[m], z_one)
        chunks(odd)

    def halve(m):
        if m:
            recv("z1_" + str(m), z1.at[m])
        else:
            recv("zn", z1.at[0, zh])
            recv("zf", z1.at[0, 1 - zh])
        other = 1 - zl // 2
        zs[m] = (pz[m, odd, other].astype(F32) + z1[m, other].astype(F32)).astype(BF)
        send("z2_" + str(m), zs.at[m], z2.at[m], z_two)

    def sum_z(m, out):
        recv("z2_" + str(m), z2.at[m])
        total = pz[m, odd, zl // 2].astype(F32) + z1[m, zl // 2].astype(F32)
        out[...] = total + z2[m].astype(F32)

    grad.finish(0)
    loads["g"].wait()
    grad.across()
    out_start(zh, "n")
    out_rest(zh, "n")

    loads["wo"].wait()

    def head_grad(z):
        total = None
        for i in range(4):
            cols = pl.ds(pl.multiple_of(z * 2560 + 640 * i, 128), 640)
            piece = mm(wo[:, cols], g_all[pl.ds(8 * z + 2 * i, 2)].reshape(640, ROWS))
            total = piece if total is None else total + piece
        return total

    hg_acc[...] = head_grad(zh)
    grad.far_sides(0)
    inp.relay()
    grad.far_sides(1)
    inp.spread(True, (1,))
    out_relay(zh, "n")
    grad.far_opposite()
    inp.forward(True, True)
    grad.finish(4)

    hg[...] = jnp.transpose(hg_acc[...] + head_grad(1 - zh)).astype(BF)
    inp.spread(False, (0, 1))

    def backward(b, carry):
        row = pl.multiple_of(b * BLOCK, BLOCK)
        for h in range(2):
            cols = pl.ds(h * HD, HD)
            rows, span = pl.ds(row, BLOCK), pl.ds(row, SPAN)
            keys, values = kcat[span, cols], vcat[span, cols]
            grads = hg[rows, cols]
            probs = p_all[h, b]
            prob_grad = mm_nt(grads, values)
            row_term = jnp.sum(
                grads.astype(F32) * att[rows, cols].astype(F32), axis=1, keepdims=True
            )
            score_grad = (probs * (prob_grad - row_term)).astype(BF)
            d_all[0, x, rows, cols] = (mm(score_grad, keys) * scaling).astype(BF)
            dk_acc[span, cols] += mm_tn(score_grad, q[rows, cols]) * scaling
            dv_acc[span, cols] += mm_tn(probs.astype(BF), grads)
        return carry

    lax.fori_loop(0, 3, backward, 0)
    halo_out[0] = dk_acc[pl.ds(PAD, WMAX)].astype(BF)
    halo_out[1] = dv_acc[pl.ds(PAD, WMAX)].astype(BF)

    send("hg", halo_out, halo_in, s_prev)
    share(1)
    out_start(1 - zh, "f")
    inp.forward(True, False)
    inp.forward(False, True)
    out_sum(zh, "n")
    recv("hg", halo_in)
    for acc, i in ((dk_acc, 0), (dv_acc, 1)):
        own = pl.ds(PAD + WMAX, ROWS - WMAX)
        last = pl.ds(PAD + ROWS, WMAX)
        d_all[1 + i, x, pl.ds(0, ROWS - WMAX)] = acc[own].astype(BF)
        d_all[1 + i, x, pl.ds(ROWS - WMAX, WMAX)] = (acc[last] + halo_in[i].astype(F32)).astype(BF)

    for name in ("wq", "wk", "wv"):
        loads[name].wait()

    def ig_chunks(core):
        def chunk(j, carry):
            y_, zh_ = j // 2, lax.rem(j, 2)
            s = slot(zh_, y_, core)
            total = mm_nt(w_all[0, s], d_all[0, x])
            total = total + mm_nt(w_all[1, s], d_all[1, x])
            total = total + mm_nt(w_all[2, s], d_all[2, x])
            igp[core, y_, zh_] = total.astype(BF)
            return carry

        lax.fori_loop(0, 8, chunk, 0)

    def add_core(j, carry):
        y_, zh_ = j // 2, lax.rem(j, 2)
        total = igp[c, y_, zh_].astype(F32) + d2r[y_, zh_].astype(F32)
        igp[c, y_, zh_] = total.astype(BF)
        return carry

    share(2)
    inp.opposite(True)
    ig_chunks(1 - c)
    send("id", igp.at[1 - c], d2r, partner)
    share_on(1)
    share(3)
    inp.forward(False, False)
    ig_chunks(c)
    inp.opposite(False)
    share_on(2)
    inp.follow()
    produce(1)
    recv("id", d2r)
    lax.fori_loop(0, 8, add_core, 0)
    send("ia", igp.at[c, yo, 0], yrel.at[0], y_right)
    send("ib", igp.at[c, yo, 1], yrel.at[1], y_left)
    send("ic", igp.at[c, yr, 1], yrec.at[0, 1], y_right)
    send("ie", igp.at[c, yl, 0], yrec.at[1, 0], y_left)
    share_on(3)
    out_rest(1 - zh, "f")
    produce(2)
    recv("ia", yrel.at[0])
    igp[c, yr, 0] = (igp[c, yr, 0].astype(F32) + yrel[0].astype(F32)).astype(BF)
    send("if", igp.at[c, yr, 0], yrec.at[0, 0], y_right)
    recv("ib", yrel.at[1])
    igp[c, yl, 1] = (igp[c, yl, 1].astype(F32) + yrel[1].astype(F32)).astype(BF)
    send("ig", igp.at[c, yl, 1], yrec.at[1, 1], y_left)
    produce(3)
    halve(1)
    out_relay(1 - zh, "f")
    halve(2)
    recv("ic", yrec.at[0, 1])
    recv("ie", yrec.at[1, 0])
    recv("if", yrec.at[0, 0])
    recv("ig", yrec.at[1, 1])
    for i in range(2):
        total = igp[c, y, i].astype(F32) + yrec[0, i].astype(F32)
        zs_ig[i] = (total + yrec[1, i].astype(F32)).astype(BF)
    send("iq", zs_ig.at[1 - zh], zr_ig.at[0], z_far)
    out_sum(1 - zh, "f")
    halve(3)
    halve(0)
    recv("iq", zr_ig.at[0])
    send("iz", zr_ig.at[0], zr_ig.at[1], zat(way))
    sum_z(1, dq_out)
    sum_z(2, dk_out)
    sum_z(3, dv_out)
    sum_z(0, do_out)
    recv("iz", zr_ig.at[1])
    ig_out[...] = (zs_ig[zh].astype(F32) + zr_ig[1].astype(F32)).astype(BF)
    inp.finish()
    wire.finish()


def leave(*refs):
    sources, targets, held = refs[:5], refs[5:10], refs[10:15]
    into, out = refs[15:]
    first = [
        pltpu.make_async_copy(s, h, into.at[i]) for i, (s, h) in enumerate(zip(sources, held))
    ]
    second = [
        pltpu.make_async_copy(h, t, out.at[i]) for i, (h, t) in enumerate(zip(held, targets))
    ]
    for cp in first:
        cp.start()
    for a, b in zip(first, second):
        a.wait()
        b.start()
    for cp in second:
        cp.wait()


def local(
    layer_input, query_rows, key_rows, value_rows, out_grad, window, w_query, w_key, w_value, w_out
):
    anywhere = pl.BlockSpec(memory_space=pl.ANY)
    vmem = pl.BlockSpec(memory_space=pltpu.VMEM)
    chunk = (SHARD, COLS)
    outs = pl.pallas_call(
        kernel,
        out_shape=(
            jax.ShapeDtypeStruct((SHARD, ROWS), BF),
            jax.ShapeDtypeStruct(chunk, F32),
            jax.ShapeDtypeStruct(chunk, F32),
            jax.ShapeDtypeStruct(chunk, F32),
            jax.ShapeDtypeStruct(chunk, F32),
        ),
        in_specs=[pl.BlockSpec(memory_space=pltpu.SMEM)] + [anywhere] * 9,
        out_specs=(vmem,) * 5,
        scratch_shapes=[
            pltpu.VMEM((16, SHARD, ROWS), BF),
            pltpu.VMEM((4, 4, SHARD, ROWS), BF),
            pltpu.VMEM((2, SHARD, ROWS), BF),
            pltpu.VMEM((3, 16) + chunk, BF),
            pltpu.VMEM((COLS, 16 * SHARD), BF),
            pltpu.VMEM((ROWS, COLS), BF),
            pltpu.VMEM((KEYS, COLS), BF),
            pltpu.VMEM((KEYS, COLS), BF),
            pltpu.VMEM((2, 3, BLOCK, SPAN), F32),
            pltpu.VMEM((ROWS, COLS), BF),
            pltpu.VMEM((ROWS, COLS), BF),
            pltpu.VMEM((COLS, ROWS), F32),
            pltpu.VMEM((3, 4, ROWS, COLS), BF),
            pltpu.VMEM((KEYS, COLS), F32),
            pltpu.VMEM((KEYS, COLS), F32),
            pltpu.VMEM((2, WMAX, COLS), BF),
            pltpu.VMEM((2, WMAX, COLS), BF),
            pltpu.VMEM((4, 2, 2) + chunk, BF),
            pltpu.VMEM((2,) + chunk, BF),
            pltpu.VMEM((2,) + chunk, BF),
            pltpu.VMEM((2, 2) + chunk, BF),
            pltpu.VMEM((2, 2) + chunk, BF),
            pltpu.VMEM((4, 2, 2) + chunk, BF),
            pltpu.VMEM((4, 2) + chunk, BF),
            pltpu.VMEM((4,) + chunk, BF),
            pltpu.VMEM((4,) + chunk, BF),
            pltpu.VMEM((2, 4, 2, SHARD, ROWS), BF),
            pltpu.VMEM((4, 2, SHARD, ROWS), BF),
            pltpu.VMEM((2, SHARD, ROWS), BF),
            pltpu.VMEM((2, 2, SHARD, ROWS), BF),
            pltpu.VMEM((2, SHARD, ROWS), BF),
            pltpu.VMEM((2, SHARD, ROWS), BF),
            pltpu.SemaphoreType.DMA((SEMS,)),
            pltpu.SemaphoreType.DMA((SEMS,)),
            pltpu.SemaphoreType.DMA((9,)),
            pltpu.SemaphoreType.DMA((2,)),
            pltpu.SemaphoreType.DMA((8,)),
        ],
        compiler_params=pltpu.CompilerParams(
            collective_id=0, has_side_effects=True, vmem_limit_bytes=66_000_000
        ),
        name="layer_backward",
    )(
        window,
        layer_input.T,
        out_grad.T,
        query_rows,
        key_rows,
        value_rows,
        w_query.reshape(16, SHARD, COLS),
        w_key.reshape(16, SHARD, COLS),
        w_value.reshape(16, SHARD, COLS),
        w_out,
    )
    shapes = tuple(jax.ShapeDtypeStruct(o.shape, o.dtype) for o in outs)
    outs = pl.pallas_call(
        leave,
        out_shape=shapes,
        in_specs=[anywhere] * 5,
        out_specs=(anywhere,) * 5,
        scratch_shapes=[pltpu.VMEM(o.shape, o.dtype) for o in outs]
        + [pltpu.SemaphoreType.DMA((5,)), pltpu.SemaphoreType.DMA((5,))],
        name="leave",
    )(*outs)
    input_grad, query_grad, key_grad, value_grad, out_grad_t = outs
    return (input_grad.T, query_grad, key_grad, value_grad, out_grad_t.T)


def solution(mesh):
    in_specs = (
        P("section", "tensor"),
        P("section", "tensor"),
        P("section", "tensor"),
        P("section", "tensor"),
        P("section", "tensor"),
        P("tensor"),
        P(None, "tensor"),
        P(None, "tensor"),
        P(None, "tensor"),
        P("tensor", None),
    )
    out_specs = (
        P("section", "tensor"),
        P("section", "tensor"),
        P("section", "tensor"),
        P("section", "tensor"),
        P("tensor", "section"),
    )
    return jax.shard_map(local, mesh=mesh, in_specs=in_specs, out_specs=out_specs, check_vma=False)
```

```python
import math

import jax
import jax.numpy as jnp
from jax import lax
from jax.experimental import pallas as pl
from jax.experimental.pallas import tpu as pltpu
from jax.sharding import PartitionSpec as P

HD = 128
WMAX = 192
ROWS = 384
COLS = 256
SHARD = 320
PAD = 64
KEYS = PAD + WMAX + ROWS
BLOCK = 128
SPAN = 384
SEMS = 160
MESH = pl.DeviceIdType.MESH
BF = jnp.bfloat16
F32 = jnp.float32


def mm(a, b):
    return jnp.dot(a, b, preferred_element_type=F32)


def mm_nt(a, b):
    return lax.dot_general(a, b, (((1,), (1,)), ((), ())), preferred_element_type=F32)


def mm_tn(a, b):
    return lax.dot_general(a, b, (((0,), (0,)), ((), ())), preferred_element_type=F32)


class Wire:
    def __init__(self, send_sem, recv_sem, someone):
        self.send_sem, self.recv_sem, self.someone = send_sem, recv_sem, someone
        self.index = {}
        self.sent = []
        self.role = None

    def copy(self, name, src, dst, device):
        i = self.index.setdefault(name, len(self.index))
        assert i < SEMS
        return pltpu.make_async_remote_copy(
            src_ref=src,
            dst_ref=dst,
            send_sem=self.send_sem.at[i],
            recv_sem=self.recv_sem.at[i],
            device_id=device,
            device_id_type=MESH,
        )

    def send(self, name, src, dst, device, like=None):
        c = self.copy(name, src, dst, device)
        c.start()
        self.sent.append((self.role, c if like is None else (name, like)))

    def only(self, role, body):
        self.role = role
        pl.when(role)(body)
        self.role = None

    def recv(self, name, dst):
        self.copy(name, dst, dst, self.someone).wait_recv()

    def finish(self):
        for role, c in self.sent:
            if role is None:
                c.wait_send()
            else:

                def body(name=c[0], like=c[1]):
                    self.copy(name, like(), like(), self.someone).wait_send()

                pl.when(role)(body)


def kernel(
    window,
    x_in,
    g_in,
    q_in,
    k_in,
    v_in,
    wq_in,
    wk_in,
    wv_in,
    wo_in,
    ig_out,
    dq_out,
    dk_out,
    dv_out,
    do_out,
    g_all,
    xg,
    z_rel,
    w_all,
    wo,
    q,
    kcat,
    vcat,
    p_all,
    att,
    hg,
    hg_acc,
    d_all,
    dk_acc,
    dv_acc,
    halo_out,
    halo_in,
    part,
    rel_l,
    rel_r,
    rec_l,
    rec_r,
    pz,
    z1,
    zs,
    z2,
    igp,
    d2r,
    yrel,
    yrec,
    zs_ig,
    zr_ig,
    send_sem,
    recv_sem,
    load_sem,
    home_send,
    home_recv,
):
    section = lax.axis_index("section")
    tensor = lax.axis_index("tensor")
    zl, x = section // 4, lax.rem(section, 4)
    zh, y, c = tensor // 8, lax.rem(tensor // 2, 4), lax.rem(tensor, 2)
    zz = zh * 4 + zl
    way = 1 - 2 * c
    xr, xo, xl = lax.rem(x + 1, 4), lax.rem(x + 2, 4), lax.rem(x + 3, 4)
    yr, yo, yl = lax.rem(y + 1, 4), lax.rem(y + 2, 4), lax.rem(y + 3, 4)

    def at(x_=x, y_=y, zz_=zz, c_=c):
        return (lax.rem(zz_, 4) * 4 + x_, (zz_ // 4) * 8 + y_ * 2 + c_)

    def slot(zh_=zh, y_=y, c_=c):
        return zh_ * 8 + y_ * 2 + c_

    def zat(step, x_=x):
        return at(x_=x_, zz_=lax.rem(zz + step + 8, 8))

    partner = at(c_=1 - c)
    y_right, y_left = at(y_=yr), at(y_=yl)
    x_right, x_left = at(x_=xr), at(x_=xl)
    z_far = zat(3 * way)
    odd = lax.rem(zl, 2)
    z_one = ((zl + 1 - 2 * odd) * 4 + x, tensor)
    z_two = (lax.rem(zl + 2, 4) * 4 + x, tensor)
    s_next = (lax.rem(section + 1, 16), tensor)
    s_prev = (lax.rem(section + 15, 16), tensor)

    home = lax.rem(y, 2) * 2 + c
    to_home = lax.rem(home - x + 4, 4)
    on_core = c == lax.rem(x, 2)
    on_chip = lax.rem(y, 2) == x // 2
    holder = jnp.logical_and(on_core, on_chip)
    middle = jnp.logical_and(on_core, jnp.logical_not(on_chip))
    follower = jnp.logical_not(on_core)
    y_a = jnp.where(on_chip, y, yl)
    y_b = jnp.where(on_chip, yo, yr)

    loads = {}

    def load(name, src, dst):
        cp = pltpu.make_async_copy(src, dst, load_sem.at[len(loads)])
        loads[name] = cp
        cp.start()

    load("q", q_in, q)
    load("k", k_in, kcat.at[pl.ds(PAD + WMAX, ROWS)])
    load("v", v_in, vcat.at[pl.ds(PAD + WMAX, ROWS)])
    load("g", g_in, g_all.at[tensor])
    load("wo", wo_in, wo)
    load("wq", wq_in, w_all.at[0])
    load("wk", wk_in, w_all.at[1])
    load("wv", wv_in, w_all.at[2])
    own_x = pltpu.make_async_copy(x_in, xg.at[zh * 2 + y // 2, x], load_sem.at[len(loads)])
    pl.when(to_home == 0)(own_x.start)

    barrier = pltpu.get_barrier_semaphore()
    peers = [partner, y_right, y_left, x_right, x_left, at(x_=xo), s_next, s_prev]
    peers += [z_one, z_two, zat(3), zat(-3)]
    peers += [zat(step, x_) for step in (1, -1) for x_ in (x, xr, xo, xl)]
    for peer in peers:
        pl.semaphore_signal(barrier, inc=1, device_id=peer, device_id_type=MESH)
    pl.semaphore_wait(barrier, len(peers))

    wire = Wire(send_sem, recv_sem, partner)
    send, recv = wire.send, wire.recv

    class Gather:
        def __init__(self, tag, own, buf, rel):
            self.tag, self.own, self.buf, self.rel = tag, own, buf, rel

        def start(self):
            def own(i):
                return self.own.at[pl.ds(160 * i, 160)]

            for i in range(2):
                send(self.tag + "L" + str(i), own(i), self.half(tensor, i), y_right)
                send(self.tag + "R" + str(i), own(1 - i), self.half(tensor, 1 - i), y_left)
                send(self.tag + "Q" + str(i), own(i), self.rel.at[pl.ds(160 * i, 160)], z_far)
            send(self.tag + "P0", self.own, self.buf.at[tensor], partner)

        def half(self, s, i):
            return self.buf.at[s, pl.ds(160 * i, 160)]

        def sides(self, z, far, names, steps):
            left, right = slot(far, yl), slot(far, yr)
            if 0 in steps:
                recv(self.tag + z + "L0", self.half(left, 0))
                send(self.tag + z + "OA", self.half(left, 0), self.half(left, 0), y_right)
                recv(self.tag + z + "R0", self.half(right, 1))
                send(self.tag + z + "OB", self.half(right, 1), self.half(right, 1), y_left)
            if 1 in steps:
                recv(self.tag + z + "L1", self.half(left, 1))
                send(self.tag + names[0], self.buf.at[left], self.buf.at[left], partner)
                recv(self.tag + z + "R1", self.half(right, 0))
                send(self.tag + names[1], self.buf.at[right], self.buf.at[right], partner)

        def opposite(self, z, far, name):
            here = slot(far, yo)
            recv(self.tag + z + "OA", self.half(here, 0))
            recv(self.tag + z + "OB", self.half(here, 1))
            send(self.tag + name, self.buf.at[here], self.buf.at[here], partner)

        def near_sides(self):
            self.sides("", zh, ("P1", "P2"), (0, 1))

        def near_opposite(self):
            self.opposite("", zh, "P3")

        def relay(self):
            source = lax.rem(zz - 3 * way + 8, 8)
            here = slot(source // 4)
            for i in range(2):
                piece = self.rel.at[pl.ds(160 * i, 160)]
                recv(self.tag + "Q" + str(i), piece)
                send(self.tag + "Z" + str(i), piece, self.half(here, i), zat(way))

        def across(self):
            here = slot(1 - zh)
            low, high = self.half(here, 0), self.half(here, 1)
            recv(self.tag + "Z0", low)
            send(self.tag + "ZL0", low, low, y_right)
            recv(self.tag + "Z1", high)
            send(self.tag + "ZR0", high, high, y_left)
            send(self.tag + "ZL1", high, high, y_right)
            send(self.tag + "ZR1", low, low, y_left)
            send(self.tag + "P4", self.buf.at[here], self.buf.at[here], partner)

        def far_sides(self, step):
            self.sides("Z", 1 - zh, ("P5", "P6"), (step,))

        def far_opposite(self):
            self.opposite("Z", 1 - zh, "P7")

        def finish(self, first):
            for i in range(first, first + 4):
                far = zh if i < 4 else 1 - zh
                where = (y, yl, yr, yo)[i % 4]
                recv(self.tag + "P" + str(i), self.buf.at[slot(far, where, 1 - c)])

    class Spread:
        def block(self, zh_, y_):
            return zh_ * 2 + y_ // 2

        def two(self):
            return xg.at[0, pl.ds(0, 2)]

        def four(self):
            return xg.at[0]

        def start(self):
            there = (zl * 4 + home, tensor)
            self.own = pltpu.make_async_remote_copy(
                src_ref=x_in,
                dst_ref=xg.at[self.block(zh, y), x],
                send_sem=home_send.at[0],
                recv_sem=home_recv.at[to_home],
                device_id=there,
                device_id_type=MESH,
            )
            pl.when(to_home != 0)(self.own.start)

        def start_far(self):
            send("xQ", x_in, z_rel.at[1], z_far)

        def relay(self):
            recv("xQ", z_rel.at[1])
            source = lax.rem(zz - 3 * way + 8, 8)
            self.far = pltpu.make_async_remote_copy(
                src_ref=z_rel.at[1],
                dst_ref=xg.at[self.block(source // 4, y), x],
                send_sem=home_send.at[1],
                recv_sem=home_recv.at[4 + to_home],
                device_id=zat(way, home),
                device_id_type=MESH,
            )
            self.far.start()

        def arrived(self, block, d, i):
            dst = xg.at[block, lax.rem(x - d + 4, 4)]
            pltpu.make_async_remote_copy(
                src_ref=dst,
                dst_ref=dst,
                send_sem=home_send.at[0],
                recv_sem=home_recv.at[i],
                device_id=partner,
                device_id_type=MESH,
            ).wait_recv()

        def spread(self, near, halves):
            tag = "xn" if near else "xf"
            far = zh if near else 1 - zh
            mine = self.block(far, y)

            def body():
                if 0 in halves:
                    if near:
                        own_x.wait()
                    else:
                        self.arrived(mine, 0, 4)
                    for d in (1, 2, 3):
                        self.arrived(mine, d, d if near else 4 + d)
                for i in halves:
                    half = xg.at[mine, pl.ds(2 * i, 2)]
                    send(tag + "L" + str(i), half, half, y_right, self.two)
                    half = xg.at[mine, pl.ds(2 - 2 * i, 2)]
                    send(tag + "R" + str(i), half, half, y_left, self.two)
                if 1 in halves:
                    send(tag + "A", xg.at[mine], xg.at[mine], partner, self.four)

            wire.only(holder, body)

        def forward(self, near, first):
            tag = "xn" if near else "xf"
            far = zh if near else 1 - zh
            left, right = self.block(far, yl), self.block(far, yr)

            def half(block, i):
                return xg.at[block, pl.ds(2 * i, 2)]

            def body():
                if first:
                    recv(tag + "L0", half(left, 0))
                    send(tag + "OA", half(left, 0), half(left, 0), y_right, self.two)
                    recv(tag + "R0", half(right, 1))
                    send(tag + "OB", half(right, 1), half(right, 1), y_left, self.two)
                else:
                    recv(tag + "L1", half(left, 1))
                    send(tag + "A", xg.at[left], xg.at[left], partner, self.four)
                    recv(tag + "R1", half(right, 0))
                    send(tag + "B", xg.at[right], xg.at[right], partner, self.four)

            wire.only(middle, body)

        def opposite(self, near):
            tag = "xn" if near else "xf"
            far = zh if near else 1 - zh
            here = self.block(far, yo)

            def body():
                recv(tag + "OA", xg.at[here, pl.ds(0, 2)])
                recv(tag + "OB", xg.at[here, pl.ds(2, 2)])
                send(tag + "B", xg.at[here], xg.at[here], partner, self.four)

            wire.only(holder, body)

        def follow(self):
            def body():
                for tag, far in (("xn", zh), ("xf", 1 - zh)):
                    recv(tag + "A", xg.at[self.block(far, y_a)])
                    recv(tag + "B", xg.at[self.block(far, y_b)])

            wire.only(follower, body)

        def finish(self):
            pl.when(to_home != 0)(self.own.wait_send)
            self.far.wait_send()

    grad = Gather("g", g_in, g_all, z_rel.at[0])
    inp = Spread()
    halo_rows = pl.ds(ROWS - WMAX, WMAX)
    grad.start()
    send("hk", k_in.at[halo_rows], kcat.at[pl.ds(PAD, WMAX)], s_next)
    send("hv", v_in.at[halo_rows], vcat.at[pl.ds(PAD, WMAX)], s_next)
    inp.start()
    grad.near_sides()
    grad.relay()
    inp.start_far()
    grad.near_opposite()
    inp.spread(True, (0,))

    scaling = 1.0 / math.sqrt(HD)
    zero_rows = jnp.zeros((PAD, COLS), BF)
    kcat[pl.ds(0, PAD)] = zero_rows
    vcat[pl.ds(0, PAD)] = zero_rows
    dk_acc[...] = jnp.zeros_like(dk_acc)
    dv_acc[...] = jnp.zeros_like(dv_acc)
    loads["q"].wait()
    loads["k"].wait()
    loads["v"].wait()
    recv("hk", kcat.at[pl.ds(PAD, WMAX)])
    recv("hv", vcat.at[pl.ds(PAD, WMAX)])
    first = section * ROWS

    def forward(b, carry):
        row = pl.multiple_of(b * BLOCK, BLOCK)
        i = lax.broadcasted_iota(jnp.int32, (BLOCK, SPAN), 0)
        j = lax.broadcasted_iota(jnp.int32, (BLOCK, SPAN), 1)
        distance = i + (PAD + WMAX) - j
        key_pos = first - (PAD + WMAX) + row + j
        for h in range(2):
            cols = pl.ds(h * HD, HD)
            keys = kcat[pl.ds(row, SPAN), cols]
            values = vcat[pl.ds(row, SPAN), cols]
            scores = mm_nt(q[pl.ds(row, BLOCK), cols], keys) * scaling
            seen = (distance >= 0) & (distance < window[h]) & (key_pos >= 0)
            scores = jnp.where(seen, scores, -1e30)
            expon = jnp.exp(scores - jnp.max(scores, axis=1, keepdims=True))
            expon = jnp.where(seen, expon, 0.0)
            probs = expon / jnp.sum(expon, axis=1, keepdims=True)
            p_all[h, b] = probs
            att[pl.ds(row, BLOCK), cols] = mm(probs.astype(BF), values).astype(BF)
        return carry

    lax.fori_loop(0, 3, forward, 0)

    def out_start(i, tag):
        def quarter(xq):
            def chunk(side, carry):
                part[xq, side, i] = mm(g_all[(i * 2 + side) * 4 + xq], att[...]).astype(BF)
                return carry

            lax.fori_loop(0, 2, chunk, 0)

        quarter(xo)
        send(tag + "a", part.at[xo, 0, i], rel_l.at[i], x_right)
        quarter(xr)
        quarter(xl)
        quarter(x)

    def out_rest(i, tag):
        send(tag + "b", part.at[xo, 1, i], rel_r.at[i], x_left)
        send(tag + "c", part.at[xr, 1, i], rec_l.at[1, i], x_right)
        send(tag + "d", part.at[xl, 0, i], rec_r.at[0, i], x_left)

    def out_relay(i, tag):
        recv(tag + "a", rel_l.at[i])
        total = part[xr, 0, i].astype(F32) + rel_l[i].astype(F32)
        part[xr, 0, i] = total.astype(BF)
        send(tag + "e", part.at[xr, 0, i], rec_l.at[0, i], x_right)
        recv(tag + "b", rel_r.at[i])
        total = part[xl, 1, i].astype(F32) + rel_r[i].astype(F32)
        part[xl, 1, i] = total.astype(BF)
        send(tag + "f", part.at[xl, 1, i], rec_r.at[1, i], x_left)

    def out_sum(i, tag):
        recv(tag + "c", rec_l.at[1, i])
        recv(tag + "d", rec_r.at[0, i])
        recv(tag + "e", rec_l.at[0, i])
        recv(tag + "f", rec_r.at[1, i])

        def chunk(side, carry):
            total = part[x, side, i].astype(F32) + rec_l[side, i].astype(F32)
            pz[0, side, i] = (total + rec_r[side, i].astype(F32)).astype(BF)
            return carry

        lax.fori_loop(0, 2, chunk, 0)
        send("z" + tag, pz.at[0, 1 - odd, i], z1.at[0, i], z_one)

    def share(m):
        mine = d_all.at[m - 1, x]
        send("aL" + str(m), mine, mine, x_right)
        send("aR" + str(m), mine, mine, x_left)

    def share_on(m):
        left, right = d_all.at[m - 1, xl], d_all.at[m - 1, xr]
        recv("aL" + str(m), left)
        half = d_all.at[m - 1, xl, pl.ds(0, 192)]
        send("aA" + str(m), half, half, x_right)
        recv("aR" + str(m), right)
        half = d_all.at[m - 1, xr, pl.ds(192, 192)]
        send("aB" + str(m), half, half, x_left)

    def produce(m):
        recv("aA" + str(m), d_all.at[m - 1, xo, pl.ds(0, 192)])
        recv("aB" + str(m), d_all.at[m - 1, xo, pl.ds(192, 192)])

        def chunks(side):
            def chunk(i, carry):
                total = mm(xg[i * 2 + side, 0], d_all[m - 1, 0])
                for r in range(1, 4):
                    total = total + mm(xg[i * 2 + side, r], d_all[m - 1, r])
                pz[m, side, i] = total.astype(BF)
                return carry

            lax.fori_loop(0, 2, chunk, 0)

        chunks(1 - odd)
        send("z1_" + str(m), pz.at[m, 1 - odd], z1.at[m], z_one)
        chunks(odd)

    def halve(m):
        if m:
            recv("z1_" + str(m), z1.at[m])
        else:
            recv("zn", z1.at[0, zh])
            recv("zf", z1.at[0, 1 - zh])
        other = 1 - zl // 2
        zs[m] = (pz[m, odd, other].astype(F32) + z1[m, other].astype(F32)).astype(BF)
        send("z2_" + str(m), zs.at[m], z2.at[m], z_two)

    def sum_z(m, out):
        recv("z2_" + str(m), z2.at[m])
        total = pz[m, odd, zl // 2].astype(F32) + z1[m, zl // 2].astype(F32)
        out[...] = total + z2[m].astype(F32)

    grad.finish(0)
    loads["g"].wait()
    grad.across()
    out_start(zh, "n")
    out_rest(zh, "n")

    loads["wo"].wait()

    def head_grad(z):
        total = None
        for i in range(4):
            cols = pl.ds(pl.multiple_of(z * 2560 + 640 * i, 128), 640)
            piece = mm(wo[:, cols], g_all[pl.ds(8 * z + 2 * i, 2)].reshape(640, ROWS))
            total = piece if total is None else total + piece
        return total

    hg_acc[...] = head_grad(zh)
    grad.far_sides(0)
    inp.relay()
    grad.far_sides(1)
    inp.spread(True, (1,))
    out_relay(zh, "n")
    grad.far_opposite()
    inp.forward(True, True)
    grad.finish(4)

    hg[...] = jnp.transpose(hg_acc[...] + head_grad(1 - zh)).astype(BF)
    inp.spread(False, (0, 1))

    def backward(b, carry):
        row = pl.multiple_of(b * BLOCK, BLOCK)
        for h in range(2):
            cols = pl.ds(h * HD, HD)
            rows, span = pl.ds(row, BLOCK), pl.ds(row, SPAN)
            keys, values = kcat[span, cols], vcat[span, cols]
            grads = hg[rows, cols]
            probs = p_all[h, b]
            prob_grad = mm_nt(grads, values)
            row_term = jnp.sum(
                grads.astype(F32) * att[rows, cols].astype(F32), axis=1, keepdims=True
            )
            score_grad = (probs * (prob_grad - row_term)).astype(BF)
            d_all[0, x, rows, cols] = (mm(score_grad, keys) * scaling).astype(BF)
            dk_acc[span, cols] += mm_tn(score_grad, q[rows, cols]) * scaling
            dv_acc[span, cols] += mm_tn(probs.astype(BF), grads)
        return carry

    lax.fori_loop(0, 3, backward, 0)
    halo_out[0] = dk_acc[pl.ds(PAD, WMAX)].astype(BF)
    halo_out[1] = dv_acc[pl.ds(PAD, WMAX)].astype(BF)

    send("hg", halo_out, halo_in, s_prev)
    share(1)
    out_start(1 - zh, "f")
    inp.forward(True, False)
    inp.forward(False, True)
    out_sum(zh, "n")
    recv("hg", halo_in)
    for acc, i in ((dk_acc, 0), (dv_acc, 1)):
        own = pl.ds(PAD + WMAX, ROWS - WMAX)
        last = pl.ds(PAD + ROWS, WMAX)
        d_all[1 + i, x, pl.ds(0, ROWS - WMAX)] = acc[own].astype(BF)
        d_all[1 + i, x, pl.ds(ROWS - WMAX, WMAX)] = (acc[last] + halo_in[i].astype(F32)).astype(BF)

    for name in ("wq", "wk", "wv"):
        loads[name].wait()

    def ig_chunks(core):
        def chunk(j, carry):
            y_, zh_ = j // 2, lax.rem(j, 2)
            s = slot(zh_, y_, core)
            total = mm_nt(w_all[0, s], d_all[0, x])
            total = total + mm_nt(w_all[1, s], d_all[1, x])
            total = total + mm_nt(w_all[2, s], d_all[2, x])
            igp[core, y_, zh_] = total.astype(BF)
            return carry

        lax.fori_loop(0, 8, chunk, 0)

    def add_core(j, carry):
        y_, zh_ = j // 2, lax.rem(j, 2)
        total = igp[c, y_, zh_].astype(F32) + d2r[y_, zh_].astype(F32)
        igp[c, y_, zh_] = total.astype(BF)
        return carry

    share(2)
    inp.opposite(True)
    ig_chunks(1 - c)
    send("id", igp.at[1 - c], d2r, partner)
    share_on(1)
    share(3)
    inp.forward(False, False)
    inp.opposite(False)
    share_on(2)
    out_rest(1 - zh, "f")
    inp.follow()
    produce(1)
    ig_chunks(c)
    recv("id", d2r)
    lax.fori_loop(0, 8, add_core, 0)
    send("ia", igp.at[c, yo, 0], yrel.at[0], y_right)
    send("ib", igp.at[c, yo, 1], yrel.at[1], y_left)
    send("ic", igp.at[c, yr, 1], yrec.at[0, 1], y_right)
    send("ie", igp.at[c, yl, 0], yrec.at[1, 0], y_left)
    share_on(3)
    produce(2)
    recv("ia", yrel.at[0])
    igp[c, yr, 0] = (igp[c, yr, 0].astype(F32) + yrel[0].astype(F32)).astype(BF)
    send("if", igp.at[c, yr, 0], yrec.at[0, 0], y_right)
    recv("ib", yrel.at[1])
    igp[c, yl, 1] = (igp[c, yl, 1].astype(F32) + yrel[1].astype(F32)).astype(BF)
    send("ig", igp.at[c, yl, 1], yrec.at[1, 1], y_left)
    out_relay(1 - zh, "f")
    halve(1)
    produce(3)
    halve(2)
    out_sum(1 - zh, "f")
    recv("ic", yrec.at[0, 1])
    recv("ie", yrec.at[1, 0])
    recv("if", yrec.at[0, 0])
    recv("ig", yrec.at[1, 1])
    for i in range(2):
        total = igp[c, y, i].astype(F32) + yrec[0, i].astype(F32)
        zs_ig[i] = (total + yrec[1, i].astype(F32)).astype(BF)
    send("iq", zs_ig.at[1 - zh], zr_ig.at[0], z_far)
    halve(3)
    halve(0)
    recv("iq", zr_ig.at[0])
    send("iz", zr_ig.at[0], zr_ig.at[1], zat(way))
    sum_z(1, dq_out)
    sum_z(2, dk_out)
    sum_z(3, dv_out)
    sum_z(0, do_out)
    recv("iz", zr_ig.at[1])
    ig_out[...] = (zs_ig[zh].astype(F32) + zr_ig[1].astype(F32)).astype(BF)
    inp.finish()
    wire.finish()


def leave(*refs):
    sources, targets, held = refs[:5], refs[5:10], refs[10:15]
    into, out = refs[15:]
    first = [
        pltpu.make_async_copy(s, h, into.at[i]) for i, (s, h) in enumerate(zip(sources, held))
    ]
    second = [
        pltpu.make_async_copy(h, t, out.at[i]) for i, (h, t) in enumerate(zip(held, targets))
    ]
    for cp in first:
        cp.start()
    for a, b in zip(first, second):
        a.wait()
        b.start()
    for cp in second:
        cp.wait()


def local(
    layer_input, query_rows, key_rows, value_rows, out_grad, window, w_query, w_key, w_value, w_out
):
    anywhere = pl.BlockSpec(memory_space=pl.ANY)
    vmem = pl.BlockSpec(memory_space=pltpu.VMEM)
    chunk = (SHARD, COLS)
    outs = pl.pallas_call(
        kernel,
        out_shape=(
            jax.ShapeDtypeStruct((SHARD, ROWS), BF),
            jax.ShapeDtypeStruct(chunk, F32),
            jax.ShapeDtypeStruct(chunk, F32),
            jax.ShapeDtypeStruct(chunk, F32),
            jax.ShapeDtypeStruct(chunk, F32),
        ),
        in_specs=[pl.BlockSpec(memory_space=pltpu.SMEM)] + [anywhere] * 9,
        out_specs=(vmem,) * 5,
        scratch_shapes=[
            pltpu.VMEM((16, SHARD, ROWS), BF),
            pltpu.VMEM((4, 4, SHARD, ROWS), BF),
            pltpu.VMEM((2, SHARD, ROWS), BF),
            pltpu.VMEM((3, 16) + chunk, BF),
            pltpu.VMEM((COLS, 16 * SHARD), BF),
            pltpu.VMEM((ROWS, COLS), BF),
            pltpu.VMEM((KEYS, COLS), BF),
            pltpu.VMEM((KEYS, COLS), BF),
            pltpu.VMEM((2, 3, BLOCK, SPAN), F32),
            pltpu.VMEM((ROWS, COLS), BF),
            pltpu.VMEM((ROWS, COLS), BF),
            pltpu.VMEM((COLS, ROWS), F32),
            pltpu.VMEM((3, 4, ROWS, COLS), BF),
            pltpu.VMEM((KEYS, COLS), F32),
            pltpu.VMEM((KEYS, COLS), F32),
            pltpu.VMEM((2, WMAX, COLS), BF),
            pltpu.VMEM((2, WMAX, COLS), BF),
            pltpu.VMEM((4, 2, 2) + chunk, BF),
            pltpu.VMEM((2,) + chunk, BF),
            pltpu.VMEM((2,) + chunk, BF),
            pltpu.VMEM((2, 2) + chunk, BF),
            pltpu.VMEM((2, 2) + chunk, BF),
            pltpu.VMEM((4, 2, 2) + chunk, BF),
            pltpu.VMEM((4, 2) + chunk, BF),
            pltpu.VMEM((4,) + chunk, BF),
            pltpu.VMEM((4,) + chunk, BF),
            pltpu.VMEM((2, 4, 2, SHARD, ROWS), BF),
            pltpu.VMEM((4, 2, SHARD, ROWS), BF),
            pltpu.VMEM((2, SHARD, ROWS), BF),
            pltpu.VMEM((2, 2, SHARD, ROWS), BF),
            pltpu.VMEM((2, SHARD, ROWS), BF),
            pltpu.VMEM((2, SHARD, ROWS), BF),
            pltpu.SemaphoreType.DMA((SEMS,)),
            pltpu.SemaphoreType.DMA((SEMS,)),
            pltpu.SemaphoreType.DMA((9,)),
            pltpu.SemaphoreType.DMA((2,)),
            pltpu.SemaphoreType.DMA((8,)),
        ],
        compiler_params=pltpu.CompilerParams(
            collective_id=0, has_side_effects=True, vmem_limit_bytes=66_000_000
        ),
        name="layer_backward",
    )(
        window,
        layer_input.T,
        out_grad.T,
        query_rows,
        key_rows,
        value_rows,
        w_query.reshape(16, SHARD, COLS),
        w_key.reshape(16, SHARD, COLS),
        w_value.reshape(16, SHARD, COLS),
        w_out,
    )
    shapes = tuple(jax.ShapeDtypeStruct(o.shape, o.dtype) for o in outs)
    outs = pl.pallas_call(
        leave,
        out_shape=shapes,
        in_specs=[anywhere] * 5,
        out_specs=(anywhere,) * 5,
        scratch_shapes=[pltpu.VMEM(o.shape, o.dtype) for o in outs]
        + [pltpu.SemaphoreType.DMA((5,)), pltpu.SemaphoreType.DMA((5,))],
        name="leave",
    )(*outs)
    input_grad, query_grad, key_grad, value_grad, out_grad_t = outs
    return (input_grad.T, query_grad, key_grad, value_grad, out_grad_t.T)


def solution(mesh):
    in_specs = (
        P("section", "tensor"),
        P("section", "tensor"),
        P("section", "tensor"),
        P("section", "tensor"),
        P("section", "tensor"),
        P("tensor"),
        P(None, "tensor"),
        P(None, "tensor"),
        P(None, "tensor"),
        P("tensor", None),
    )
    out_specs = (
        P("section", "tensor"),
        P("section", "tensor"),
        P("section", "tensor"),
        P("section", "tensor"),
        P("tensor", "section"),
    )
    return jax.shard_map(local, mesh=mesh, in_specs=in_specs, out_specs=out_specs, check_vma=False)
```

```python
import math

import jax
import jax.numpy as jnp
from jax import lax
from jax.experimental import pallas as pl
from jax.experimental.pallas import tpu as pltpu
from jax.sharding import PartitionSpec as P

HD = 128
WMAX = 192
ROWS = 384
COLS = 256
SHARD = 320
PAD = 64
KEYS = PAD + WMAX + ROWS
BLOCK = 128
SPAN = 384
SEMS = 160
MESH = pl.DeviceIdType.MESH
BF = jnp.bfloat16
F32 = jnp.float32


def mm(a, b):
    return jnp.dot(a, b, preferred_element_type=F32)


def mm_nt(a, b):
    return lax.dot_general(a, b, (((1,), (1,)), ((), ())), preferred_element_type=F32)


def mm_tn(a, b):
    return lax.dot_general(a, b, (((0,), (0,)), ((), ())), preferred_element_type=F32)


class Wire:
    def __init__(self, send_sem, recv_sem, someone):
        self.send_sem, self.recv_sem, self.someone = send_sem, recv_sem, someone
        self.index = {}
        self.sent = []
        self.role = None

    def copy(self, name, src, dst, device):
        i = self.index.setdefault(name, len(self.index))
        assert i < SEMS
        return pltpu.make_async_remote_copy(
            src_ref=src,
            dst_ref=dst,
            send_sem=self.send_sem.at[i],
            recv_sem=self.recv_sem.at[i],
            device_id=device,
            device_id_type=MESH,
        )

    def send(self, name, src, dst, device, like=None):
        c = self.copy(name, src, dst, device)
        c.start()
        self.sent.append((self.role, c if like is None else (name, like)))

    def only(self, role, body):
        self.role = role
        pl.when(role)(body)
        self.role = None

    def recv(self, name, dst):
        self.copy(name, dst, dst, self.someone).wait_recv()

    def finish(self):
        for role, c in self.sent:
            if role is None:
                c.wait_send()
            else:

                def body(name=c[0], like=c[1]):
                    self.copy(name, like(), like(), self.someone).wait_send()

                pl.when(role)(body)


def kernel(
    window,
    x_in,
    g_in,
    q_in,
    k_in,
    v_in,
    wq_in,
    wk_in,
    wv_in,
    wo_in,
    ig_out,
    dq_out,
    dk_out,
    dv_out,
    do_out,
    g_all,
    xg,
    z_rel,
    w_all,
    wo,
    q,
    kcat,
    vcat,
    p_all,
    att,
    hg,
    hg_acc,
    d_all,
    dk_acc,
    dv_acc,
    halo_out,
    halo_in,
    part,
    rel_l,
    rel_r,
    rec_l,
    rec_r,
    pz,
    z1,
    zs,
    z2,
    igp,
    d2r,
    yrel,
    yrec,
    zs_ig,
    zr_ig,
    send_sem,
    recv_sem,
    load_sem,
    home_send,
    home_recv,
):
    section = lax.axis_index("section")
    tensor = lax.axis_index("tensor")
    zl, x = section // 4, lax.rem(section, 4)
    zh, y, c = tensor // 8, lax.rem(tensor // 2, 4), lax.rem(tensor, 2)
    zz = zh * 4 + zl
    way = 1 - 2 * c
    xr, xo, xl = lax.rem(x + 1, 4), lax.rem(x + 2, 4), lax.rem(x + 3, 4)
    yr, yo, yl = lax.rem(y + 1, 4), lax.rem(y + 2, 4), lax.rem(y + 3, 4)

    def at(x_=x, y_=y, zz_=zz, c_=c):
        return (lax.rem(zz_, 4) * 4 + x_, (zz_ // 4) * 8 + y_ * 2 + c_)

    def slot(zh_=zh, y_=y, c_=c):
        return zh_ * 8 + y_ * 2 + c_

    def zat(step, x_=x):
        return at(x_=x_, zz_=lax.rem(zz + step + 8, 8))

    partner = at(c_=1 - c)
    y_right, y_left = at(y_=yr), at(y_=yl)
    x_right, x_left = at(x_=xr), at(x_=xl)
    z_far = zat(3 * way)
    odd = lax.rem(zl, 2)
    z_one = ((zl + 1 - 2 * odd) * 4 + x, tensor)
    z_two = (lax.rem(zl + 2, 4) * 4 + x, tensor)
    s_next = (lax.rem(section + 1, 16), tensor)
    s_prev = (lax.rem(section + 15, 16), tensor)

    home = lax.rem(y, 2) * 2 + c
    to_home = lax.rem(home - x + 4, 4)
    on_core = c == lax.rem(x, 2)
    on_chip = lax.rem(y, 2) == x // 2
    holder = jnp.logical_and(on_core, on_chip)
    middle = jnp.logical_and(on_core, jnp.logical_not(on_chip))
    follower = jnp.logical_not(on_core)
    y_a = jnp.where(on_chip, y, yl)
    y_b = jnp.where(on_chip, yo, yr)

    loads = {}

    def load(name, src, dst):
        cp = pltpu.make_async_copy(src, dst, load_sem.at[len(loads)])
        loads[name] = cp
        cp.start()

    load("q", q_in, q)
    load("k", k_in, kcat.at[pl.ds(PAD + WMAX, ROWS)])
    load("v", v_in, vcat.at[pl.ds(PAD + WMAX, ROWS)])
    load("g", g_in, g_all.at[tensor])
    load("wo", wo_in, wo)
    load("wq", wq_in, w_all.at[0])
    load("wk", wk_in, w_all.at[1])
    load("wv", wv_in, w_all.at[2])
    own_x = pltpu.make_async_copy(x_in, xg.at[zh * 2 + y // 2, x], load_sem.at[len(loads)])
    pl.when(to_home == 0)(own_x.start)

    barrier = pltpu.get_barrier_semaphore()
    peers = [partner, y_right, y_left, x_right, x_left, at(x_=xo), s_next, s_prev]
    peers += [z_one, z_two, zat(3), zat(-3)]
    peers += [zat(step, x_) for step in (1, -1) for x_ in (x, xr, xo, xl)]
    for peer in peers:
        pl.semaphore_signal(barrier, inc=1, device_id=peer, device_id_type=MESH)
    pl.semaphore_wait(barrier, len(peers))

    wire = Wire(send_sem, recv_sem, partner)
    send, recv = wire.send, wire.recv

    class Gather:
        def __init__(self, tag, own, buf, rel):
            self.tag, self.own, self.buf, self.rel = tag, own, buf, rel

        def start(self):
            def own(i):
                return self.own.at[pl.ds(160 * i, 160)]

            for i in range(2):
                send(self.tag + "L" + str(i), own(i), self.half(tensor, i), y_right)
                send(self.tag + "R" + str(i), own(1 - i), self.half(tensor, 1 - i), y_left)
                send(self.tag + "Q" + str(i), own(i), self.rel.at[pl.ds(160 * i, 160)], z_far)
            send(self.tag + "P0", self.own, self.buf.at[tensor], partner)

        def half(self, s, i):
            return self.buf.at[s, pl.ds(160 * i, 160)]

        def sides(self, z, far, names, steps):
            left, right = slot(far, yl), slot(far, yr)
            if 0 in steps:
                recv(self.tag + z + "L0", self.half(left, 0))
                send(self.tag + z + "OA", self.half(left, 0), self.half(left, 0), y_right)
                recv(self.tag + z + "R0", self.half(right, 1))
                send(self.tag + z + "OB", self.half(right, 1), self.half(right, 1), y_left)
            if 1 in steps:
                recv(self.tag + z + "L1", self.half(left, 1))
                send(self.tag + names[0], self.buf.at[left], self.buf.at[left], partner)
                recv(self.tag + z + "R1", self.half(right, 0))
                send(self.tag + names[1], self.buf.at[right], self.buf.at[right], partner)

        def opposite(self, z, far, name):
            here = slot(far, yo)
            recv(self.tag + z + "OA", self.half(here, 0))
            recv(self.tag + z + "OB", self.half(here, 1))
            send(self.tag + name, self.buf.at[here], self.buf.at[here], partner)

        def near_sides(self):
            self.sides("", zh, ("P1", "P2"), (0, 1))

        def near_opposite(self):
            self.opposite("", zh, "P3")

        def relay(self):
            source = lax.rem(zz - 3 * way + 8, 8)
            here = slot(source // 4)
            for i in range(2):
                piece = self.rel.at[pl.ds(160 * i, 160)]
                recv(self.tag + "Q" + str(i), piece)
                send(self.tag + "Z" + str(i), piece, self.half(here, i), zat(way))

        def across(self):
            here = slot(1 - zh)
            low, high = self.half(here, 0), self.half(here, 1)
            recv(self.tag + "Z0", low)
            send(self.tag + "ZL0", low, low, y_right)
            recv(self.tag + "Z1", high)
            send(self.tag + "ZR0", high, high, y_left)
            send(self.tag + "ZL1", high, high, y_right)
            send(self.tag + "ZR1", low, low, y_left)
            send(self.tag + "P4", self.buf.at[here], self.buf.at[here], partner)

        def far_sides(self, step):
            self.sides("Z", 1 - zh, ("P5", "P6"), (step,))

        def far_opposite(self):
            self.opposite("Z", 1 - zh, "P7")

        def finish(self, first):
            for i in range(first, first + 4):
                far = zh if i < 4 else 1 - zh
                where = (y, yl, yr, yo)[i % 4]
                recv(self.tag + "P" + str(i), self.buf.at[slot(far, where, 1 - c)])

    class Spread:
        def block(self, zh_, y_):
            return zh_ * 2 + y_ // 2

        def two(self):
            return xg.at[0, pl.ds(0, 2)]

        def four(self):
            return xg.at[0]

        def start(self):
            there = (zl * 4 + home, tensor)
            self.own = pltpu.make_async_remote_copy(
                src_ref=x_in,
                dst_ref=xg.at[self.block(zh, y), x],
                send_sem=home_send.at[0],
                recv_sem=home_recv.at[to_home],
                device_id=there,
                device_id_type=MESH,
            )
            pl.when(to_home != 0)(self.own.start)

        def start_far(self):
            send("xQ", x_in, z_rel.at[1], z_far)

        def relay(self):
            recv("xQ", z_rel.at[1])
            source = lax.rem(zz - 3 * way + 8, 8)
            self.far = pltpu.make_async_remote_copy(
                src_ref=z_rel.at[1],
                dst_ref=xg.at[self.block(source // 4, y), x],
                send_sem=home_send.at[1],
                recv_sem=home_recv.at[4 + to_home],
                device_id=zat(way, home),
                device_id_type=MESH,
            )
            self.far.start()

        def arrived(self, block, d, i):
            dst = xg.at[block, lax.rem(x - d + 4, 4)]
            pltpu.make_async_remote_copy(
                src_ref=dst,
                dst_ref=dst,
                send_sem=home_send.at[0],
                recv_sem=home_recv.at[i],
                device_id=partner,
                device_id_type=MESH,
            ).wait_recv()

        def spread(self, near, halves):
            tag = "xn" if near else "xf"
            far = zh if near else 1 - zh
            mine = self.block(far, y)

            def body():
                if 0 in halves:
                    if near:
                        own_x.wait()
                    else:
                        self.arrived(mine, 0, 4)
                    for d in (1, 2, 3):
                        self.arrived(mine, d, d if near else 4 + d)
                for i in halves:
                    half = xg.at[mine, pl.ds(2 * i, 2)]
                    send(tag + "L" + str(i), half, half, y_right, self.two)
                    half = xg.at[mine, pl.ds(2 - 2 * i, 2)]
                    send(tag + "R" + str(i), half, half, y_left, self.two)
                if 1 in halves:
                    send(tag + "A", xg.at[mine], xg.at[mine], partner, self.four)

            wire.only(holder, body)

        def forward(self, near, first):
            tag = "xn" if near else "xf"
            far = zh if near else 1 - zh
            left, right = self.block(far, yl), self.block(far, yr)

            def half(block, i):
                return xg.at[block, pl.ds(2 * i, 2)]

            def body():
                if first:
                    recv(tag + "L0", half(left, 0))
                    send(tag + "OA", half(left, 0), half(left, 0), y_right, self.two)
                    recv(tag + "R0", half(right, 1))
                    send(tag + "OB", half(right, 1), half(right, 1), y_left, self.two)
                else:
                    recv(tag + "L1", half(left, 1))
                    send(tag + "A", xg.at[left], xg.at[left], partner, self.four)
                    recv(tag + "R1", half(right, 0))
                    send(tag + "B", xg.at[right], xg.at[right], partner, self.four)

            wire.only(middle, body)

        def opposite(self, near):
            tag = "xn" if near else "xf"
            far = zh if near else 1 - zh
            here = self.block(far, yo)

            def body():
                recv(tag + "OA", xg.at[here, pl.ds(0, 2)])
                recv(tag + "OB", xg.at[here, pl.ds(2, 2)])
                send(tag + "B", xg.at[here], xg.at[here], partner, self.four)

            wire.only(holder, body)

        def follow(self):
            def body():
                for tag, far in (("xn", zh), ("xf", 1 - zh)):
                    recv(tag + "A", xg.at[self.block(far, y_a)])
                    recv(tag + "B", xg.at[self.block(far, y_b)])

            wire.only(follower, body)

        def finish(self):
            pl.when(to_home != 0)(self.own.wait_send)
            self.far.wait_send()

    grad = Gather("g", g_in, g_all, z_rel.at[0])
    inp = Spread()
    halo_rows = pl.ds(ROWS - WMAX, WMAX)
    grad.start()
    send("hk", k_in.at[halo_rows], kcat.at[pl.ds(PAD, WMAX)], s_next)
    send("hv", v_in.at[halo_rows], vcat.at[pl.ds(PAD, WMAX)], s_next)
    inp.start()
    grad.near_sides()
    grad.relay()
    inp.start_far()
    grad.near_opposite()
    inp.spread(True, (0,))

    scaling = 1.0 / math.sqrt(HD)
    zero_rows = jnp.zeros((PAD, COLS), BF)
    kcat[pl.ds(0, PAD)] = zero_rows
    vcat[pl.ds(0, PAD)] = zero_rows
    dk_acc[...] = jnp.zeros_like(dk_acc)
    dv_acc[...] = jnp.zeros_like(dv_acc)
    loads["q"].wait()
    loads["k"].wait()
    loads["v"].wait()
    recv("hk", kcat.at[pl.ds(PAD, WMAX)])
    recv("hv", vcat.at[pl.ds(PAD, WMAX)])
    first = section * ROWS

    def forward(b, carry):
        row = pl.multiple_of(b * BLOCK, BLOCK)
        i = lax.broadcasted_iota(jnp.int32, (BLOCK, SPAN), 0)
        j = lax.broadcasted_iota(jnp.int32, (BLOCK, SPAN), 1)
        distance = i + (PAD + WMAX) - j
        key_pos = first - (PAD + WMAX) + row + j
        for h in range(2):
            cols = pl.ds(h * HD, HD)
            keys = kcat[pl.ds(row, SPAN), cols]
            values = vcat[pl.ds(row, SPAN), cols]
            scores = mm_nt(q[pl.ds(row, BLOCK), cols], keys) * scaling
            seen = (distance >= 0) & (distance < window[h]) & (key_pos >= 0)
            scores = jnp.where(seen, scores, -1e30)
            expon = jnp.exp(scores - jnp.max(scores, axis=1, keepdims=True))
            expon = jnp.where(seen, expon, 0.0)
            probs = expon / jnp.sum(expon, axis=1, keepdims=True)
            p_all[h, b] = probs
            att[pl.ds(row, BLOCK), cols] = mm(probs.astype(BF), values).astype(BF)
        return carry

    lax.fori_loop(0, 3, forward, 0)

    def out_start(i, tag):
        def quarter(xq):
            def chunk(side, carry):
                part[xq, side, i] = mm(g_all[(i * 2 + side) * 4 + xq], att[...]).astype(BF)
                return carry

            lax.fori_loop(0, 2, chunk, 0)

        quarter(xo)
        send(tag + "a", part.at[xo, 0, i], rel_l.at[i], x_right)
        quarter(xr)
        quarter(xl)
        quarter(x)

    def out_rest(i, tag):
        send(tag + "b", part.at[xo, 1, i], rel_r.at[i], x_left)
        send(tag + "c", part.at[xr, 1, i], rec_l.at[1, i], x_right)
        send(tag + "d", part.at[xl, 0, i], rec_r.at[0, i], x_left)

    def out_relay(i, tag):
        recv(tag + "a", rel_l.at[i])
        total = part[xr, 0, i].astype(F32) + rel_l[i].astype(F32)
        part[xr, 0, i] = total.astype(BF)
        send(tag + "e", part.at[xr, 0, i], rec_l.at[0, i], x_right)
        recv(tag + "b", rel_r.at[i])
        total = part[xl, 1, i].astype(F32) + rel_r[i].astype(F32)
        part[xl, 1, i] = total.astype(BF)
        send(tag + "f", part.at[xl, 1, i], rec_r.at[1, i], x_left)

    def out_sum(i, tag):
        recv(tag + "c", rec_l.at[1, i])
        recv(tag + "d", rec_r.at[0, i])
        recv(tag + "e", rec_l.at[0, i])
        recv(tag + "f", rec_r.at[1, i])

        def chunk(side, carry):
            total = part[x, side, i].astype(F32) + rec_l[side, i].astype(F32)
            pz[0, side, i] = (total + rec_r[side, i].astype(F32)).astype(BF)
            return carry

        lax.fori_loop(0, 2, chunk, 0)
        send("z" + tag, pz.at[0, 1 - odd, i], z1.at[0, i], z_one)

    def share(m):
        mine = d_all.at[m - 1, x]
        send("aL" + str(m), mine, mine, x_right)
        send("aR" + str(m), mine, mine, x_left)

    def share_on(m):
        left, right = d_all.at[m - 1, xl], d_all.at[m - 1, xr]
        recv("aL" + str(m), left)
        half = d_all.at[m - 1, xl, pl.ds(0, 192)]
        send("aA" + str(m), half, half, x_right)
        recv("aR" + str(m), right)
        half = d_all.at[m - 1, xr, pl.ds(192, 192)]
        send("aB" + str(m), half, half, x_left)

    def produce(m):
        recv("aA" + str(m), d_all.at[m - 1, xo, pl.ds(0, 192)])
        recv("aB" + str(m), d_all.at[m - 1, xo, pl.ds(192, 192)])

        def chunks(side):
            def chunk(i, carry):
                total = mm(xg[i * 2 + side, 0], d_all[m - 1, 0])
                for r in range(1, 4):
                    total = total + mm(xg[i * 2 + side, r], d_all[m - 1, r])
                pz[m, side, i] = total.astype(BF)
                return carry

            lax.fori_loop(0, 2, chunk, 0)

        chunks(1 - odd)
        send("z1_" + str(m), pz.at[m, 1 - odd], z1.at[m], z_one)
        chunks(odd)

    def halve(m):
        if m:
            recv("z1_" + str(m), z1.at[m])
        else:
            recv("zn", z1.at[0, zh])
            recv("zf", z1.at[0, 1 - zh])
        other = 1 - zl // 2
        zs[m] = (pz[m, odd, other].astype(F32) + z1[m, other].astype(F32)).astype(BF)
        send("z2_" + str(m), zs.at[m], z2.at[m], z_two)

    def sum_z(m, out):
        recv("z2_" + str(m), z2.at[m])
        total = pz[m, odd, zl // 2].astype(F32) + z1[m, zl // 2].astype(F32)
        out[...] = total + z2[m].astype(F32)

    grad.finish(0)
    loads["g"].wait()
    grad.across()
    out_start(zh, "n")
    out_rest(zh, "n")

    loads["wo"].wait()

    def head_grad(z):
        total = None
        for i in range(4):
            cols = pl.ds(pl.multiple_of(z * 2560 + 640 * i, 128), 640)
            piece = mm(wo[:, cols], g_all[pl.ds(8 * z + 2 * i, 2)].reshape(640, ROWS))
            total = piece if total is None else total + piece
        return total

    hg_acc[...] = head_grad(zh)
    grad.far_sides(0)
    inp.relay()
    grad.far_sides(1)
    inp.spread(True, (1,))
    out_relay(zh, "n")
    grad.far_opposite()
    inp.forward(True, True)
    grad.finish(4)

    hg[...] = jnp.transpose(hg_acc[...] + head_grad(1 - zh)).astype(BF)
    inp.spread(False, (0, 1))

    def backward(b, carry):
        row = pl.multiple_of(b * BLOCK, BLOCK)
        for h in range(2):
            cols = pl.ds(h * HD, HD)
            rows, span = pl.ds(row, BLOCK), pl.ds(row, SPAN)
            keys, values = kcat[span, cols], vcat[span, cols]
            grads = hg[rows, cols]
            probs = p_all[h, b]
            prob_grad = mm_nt(grads, values)
            row_term = jnp.sum(
                grads.astype(F32) * att[rows, cols].astype(F32), axis=1, keepdims=True
            )
            score_grad = (probs * (prob_grad - row_term)).astype(BF)
            d_all[0, x, rows, cols] = (mm(score_grad, keys) * scaling).astype(BF)
            dk_acc[span, cols] += mm_tn(score_grad, q[rows, cols]) * scaling
            dv_acc[span, cols] += mm_tn(probs.astype(BF), grads)
        return carry

    lax.fori_loop(0, 3, backward, 0)
    halo_out[0] = dk_acc[pl.ds(PAD, WMAX)].astype(BF)
    halo_out[1] = dv_acc[pl.ds(PAD, WMAX)].astype(BF)

    send("hg", halo_out, halo_in, s_prev)
    share(1)
    out_start(1 - zh, "f")
    inp.forward(True, False)
    inp.forward(False, True)
    out_sum(zh, "n")
    recv("hg", halo_in)
    for acc, i in ((dk_acc, 0), (dv_acc, 1)):
        own = pl.ds(PAD + WMAX, ROWS - WMAX)
        last = pl.ds(PAD + ROWS, WMAX)
        d_all[1 + i, x, pl.ds(0, ROWS - WMAX)] = acc[own].astype(BF)
        d_all[1 + i, x, pl.ds(ROWS - WMAX, WMAX)] = (acc[last] + halo_in[i].astype(F32)).astype(BF)

    for name in ("wq", "wk", "wv"):
        loads[name].wait()

    def ig_chunks(core):
        def chunk(j, carry):
            y_, zh_ = j // 2, lax.rem(j, 2)
            s = slot(zh_, y_, core)
            total = mm_nt(w_all[0, s], d_all[0, x])
            total = total + mm_nt(w_all[1, s], d_all[1, x])
            total = total + mm_nt(w_all[2, s], d_all[2, x])
            igp[core, y_, zh_] = total.astype(BF)
            return carry

        lax.fori_loop(0, 8, chunk, 0)

    def add_core(j, carry):
        y_, zh_ = j // 2, lax.rem(j, 2)
        total = igp[c, y_, zh_].astype(F32) + d2r[y_, zh_].astype(F32)
        igp[c, y_, zh_] = total.astype(BF)
        return carry

    share(2)
    inp.opposite(True)
    ig_chunks(1 - c)
    send("id", igp.at[1 - c], d2r, partner)
    share_on(1)
    share(3)
    inp.forward(False, False)
    inp.opposite(False)
    share_on(2)
    out_rest(1 - zh, "f")
    inp.follow()
    produce(1)
    ig_chunks(c)
    recv("id", d2r)
    lax.fori_loop(0, 8, add_core, 0)
    send("ia", igp.at[c, yo, 0], yrel.at[0], y_right)
    send("ib", igp.at[c, yo, 1], yrel.at[1], y_left)
    send("ic", igp.at[c, yr, 1], yrec.at[0, 1], y_right)
    send("ie", igp.at[c, yl, 0], yrec.at[1, 0], y_left)
    share_on(3)
    produce(2)
    out_relay(1 - zh, "f")
    halve(1)
    recv("ia", yrel.at[0])
    igp[c, yr, 0] = (igp[c, yr, 0].astype(F32) + yrel[0].astype(F32)).astype(BF)
    send("if", igp.at[c, yr, 0], yrec.at[0, 0], y_right)
    recv("ib", yrel.at[1])
    igp[c, yl, 1] = (igp[c, yl, 1].astype(F32) + yrel[1].astype(F32)).astype(BF)
    send("ig", igp.at[c, yl, 1], yrec.at[1, 1], y_left)
    produce(3)
    halve(2)
    out_sum(1 - zh, "f")
    recv("ic", yrec.at[0, 1])
    recv("ie", yrec.at[1, 0])
    recv("if", yrec.at[0, 0])
    recv("ig", yrec.at[1, 1])
    for i in range(2):
        total = igp[c, y, i].astype(F32) + yrec[0, i].astype(F32)
        zs_ig[i] = (total + yrec[1, i].astype(F32)).astype(BF)
    send("iq", zs_ig.at[1 - zh], zr_ig.at[0], z_far)
    halve(3)
    halve(0)
    recv("iq", zr_ig.at[0])
    send("iz", zr_ig.at[0], zr_ig.at[1], zat(way))
    sum_z(1, dq_out)
    sum_z(2, dk_out)
    sum_z(3, dv_out)
    sum_z(0, do_out)
    recv("iz", zr_ig.at[1])
    ig_out[...] = (zs_ig[zh].astype(F32) + zr_ig[1].astype(F32)).astype(BF)
    inp.finish()
    wire.finish()


def leave(*refs):
    sources, targets, held = refs[:5], refs[5:10], refs[10:15]
    into, out = refs[15:]
    first = [
        pltpu.make_async_copy(s, h, into.at[i]) for i, (s, h) in enumerate(zip(sources, held))
    ]
    second = [
        pltpu.make_async_copy(h, t, out.at[i]) for i, (h, t) in enumerate(zip(held, targets))
    ]
    for cp in first:
        cp.start()
    for a, b in zip(first, second):
        a.wait()
        b.start()
    for cp in second:
        cp.wait()


def local(
    layer_input, query_rows, key_rows, value_rows, out_grad, window, w_query, w_key, w_value, w_out
):
    anywhere = pl.BlockSpec(memory_space=pl.ANY)
    vmem = pl.BlockSpec(memory_space=pltpu.VMEM)
    chunk = (SHARD, COLS)
    outs = pl.pallas_call(
        kernel,
        out_shape=(
            jax.ShapeDtypeStruct((SHARD, ROWS), BF),
            jax.ShapeDtypeStruct(chunk, F32),
            jax.ShapeDtypeStruct(chunk, F32),
            jax.ShapeDtypeStruct(chunk, F32),
            jax.ShapeDtypeStruct(chunk, F32),
        ),
        in_specs=[pl.BlockSpec(memory_space=pltpu.SMEM)] + [anywhere] * 9,
        out_specs=(vmem,) * 5,
        scratch_shapes=[
            pltpu.VMEM((16, SHARD, ROWS), BF),
            pltpu.VMEM((4, 4, SHARD, ROWS), BF),
            pltpu.VMEM((2, SHARD, ROWS), BF),
            pltpu.VMEM((3, 16) + chunk, BF),
            pltpu.VMEM((COLS, 16 * SHARD), BF),
            pltpu.VMEM((ROWS, COLS), BF),
            pltpu.VMEM((KEYS, COLS), BF),
            pltpu.VMEM((KEYS, COLS), BF),
            pltpu.VMEM((2, 3, BLOCK, SPAN), F32),
            pltpu.VMEM((ROWS, COLS), BF),
            pltpu.VMEM((ROWS, COLS), BF),
            pltpu.VMEM((COLS, ROWS), F32),
            pltpu.VMEM((3, 4, ROWS, COLS), BF),
            pltpu.VMEM((KEYS, COLS), F32),
            pltpu.VMEM((KEYS, COLS), F32),
            pltpu.VMEM((2, WMAX, COLS), BF),
            pltpu.VMEM((2, WMAX, COLS), BF),
            pltpu.VMEM((4, 2, 2) + chunk, BF),
            pltpu.VMEM((2,) + chunk, BF),
            pltpu.VMEM((2,) + chunk, BF),
            pltpu.VMEM((2, 2) + chunk, BF),
            pltpu.VMEM((2, 2) + chunk, BF),
            pltpu.VMEM((4, 2, 2) + chunk, BF),
            pltpu.VMEM((4, 2) + chunk, BF),
            pltpu.VMEM((4,) + chunk, BF),
            pltpu.VMEM((4,) + chunk, BF),
            pltpu.VMEM((2, 4, 2, SHARD, ROWS), BF),
            pltpu.VMEM((4, 2, SHARD, ROWS), BF),
            pltpu.VMEM((2, SHARD, ROWS), BF),
            pltpu.VMEM((2, 2, SHARD, ROWS), BF),
            pltpu.VMEM((2, SHARD, ROWS), BF),
            pltpu.VMEM((2, SHARD, ROWS), BF),
            pltpu.SemaphoreType.DMA((SEMS,)),
            pltpu.SemaphoreType.DMA((SEMS,)),
            pltpu.SemaphoreType.DMA((9,)),
            pltpu.SemaphoreType.DMA((2,)),
            pltpu.SemaphoreType.DMA((8,)),
        ],
        compiler_params=pltpu.CompilerParams(
            collective_id=0, has_side_effects=True, vmem_limit_bytes=66_000_000
        ),
        name="layer_backward",
    )(
        window,
        layer_input.T,
        out_grad.T,
        query_rows,
        key_rows,
        value_rows,
        w_query.reshape(16, SHARD, COLS),
        w_key.reshape(16, SHARD, COLS),
        w_value.reshape(16, SHARD, COLS),
        w_out,
    )
    shapes = tuple(jax.ShapeDtypeStruct(o.shape, o.dtype) for o in outs)
    outs = pl.pallas_call(
        leave,
        out_shape=shapes,
        in_specs=[anywhere] * 5,
        out_specs=(anywhere,) * 5,
        scratch_shapes=[pltpu.VMEM(o.shape, o.dtype) for o in outs]
        + [pltpu.SemaphoreType.DMA((5,)), pltpu.SemaphoreType.DMA((5,))],
        name="leave",
    )(*outs)
    input_grad, query_grad, key_grad, value_grad, out_grad_t = outs
    return (input_grad.T, query_grad, key_grad, value_grad, out_grad_t.T)


def solution(mesh):
    in_specs = (
        P("section", "tensor"),
        P("section", "tensor"),
        P("section", "tensor"),
        P("section", "tensor"),
        P("section", "tensor"),
        P("tensor"),
        P(None, "tensor"),
        P(None, "tensor"),
        P(None, "tensor"),
        P("tensor", None),
    )
    out_specs = (
        P("section", "tensor"),
        P("section", "tensor"),
        P("section", "tensor"),
        P("section", "tensor"),
        P("tensor", "section"),
    )
    return jax.shard_map(local, mesh=mesh, in_specs=in_specs, out_specs=out_specs, check_vma=False)
```
